128 devices in a mesh: freq: 64 (over x, y, z_hi, core), depth: 2 (over z_lo).
Axes of the slice: x: 4, y: 4, z: 4 (z_hi: 2, z_lo: 2; z = z_hi * 2 + z_lo), core: 2. Of those that a mesh axis runs over, the one named last changes fastest.
Arguments:
- pressure_field: bfloat16 [8192, 16384], P('depth', 'freq'), may hold values from -6 to 6
- block_main: bfloat16 [8192, 3, 2, 128], P('depth'), may hold values from -0.15625 to 0.15625
- block_coupled: bfloat16 [8192, 3, 2, 128], P('depth'), may hold values from -0.15625 to 0.15625
- coupling: float32 [16384], P('freq'), may hold values from -3 to 3
- frequencies: float32 [8192], replicated, may hold values from 1 to 1024
- receivers: int32 [512], replicated, may hold values from 0 to 8191
- floors: int32 [4], replicated, may hold values from 2048 to 8191
Outputs:
- series: float32 [512, 2048], P('depth', 'freq')
The draws below stay inside these ranges and needn't reach their ends.
Inputs may be any that keep to these rules, and one draw needn't show every extreme that they name: `receivers`: any depth cells, repeats possible.
All inputs are finite; a program needn't handle non-finite values.
Results may differ from the reference program's by a relative error of at most 0.0061.
Values may be sent and summed in bfloat16 or wider, within the bound.
A program may use at most 256 MiB of HBM per device.

```python
import math
import jax
import jax.numpy as jnp
from jax import lax

NZ = 8192
BS = 128
NT = 2048
R = 512
STEPS = 4
F_DEV = 128
F = 8192
N_FREQ = 64


def touch_ends(array, key, smallest, largest):
    index_at = [jax.random.randint(jax.random.fold_in(key, axis), (), 0, length) for axis, length in enumerate(array.shape)]
    main_axis = array.shape.index(max(array.shape))
    next_to = index_at[:main_axis] + [(index_at[main_axis] + 1) % array.shape[main_axis]] + index_at[main_axis + 1:]
    return array.at[tuple(index_at)].set(smallest).at[tuple(next_to)].set(largest)


def levels(own_key, shape, cuts, least, top_value):
    level = 1.0
    for position, blocks in cuts:
        draws = jax.random.uniform(jax.random.fold_in(jax.random.fold_in(own_key, 6), position), (blocks,), jnp.float32, least / len(cuts), top_value / len(cuts))
        level = level * jnp.repeat(jnp.exp(draws), shape[position] // blocks).reshape((-1,) + (1,) * (len(shape) - 1 - position))
    return level


def gaussian(stream_key, dims, scale, reach, split=(), held_as=jnp.bfloat16):
    entries = scale * jax.random.normal(stream_key, dims, jnp.float32)
    if split:
        entries = entries * levels(stream_key, dims, split, -0.22, 0.18)
    return jnp.clip(entries, -reach, reach).astype(held_as)


def setup_inputs(seed: int = 0) -> dict:
    streams_of = jax.random.split(jax.random.key(seed), 8)
    return {
        "pressure_field": gaussian(streams_of[0], (NZ, 2 * F), 1.0, 6.0, ((0, 2), (1, 64))),
        "block_main": gaussian(streams_of[1], (NZ, 3, 2, BS), (12 * BS) ** -0.5, 0.15625, ((0, 2),)),
        "block_coupled": gaussian(streams_of[2], (NZ, 3, 2, BS), (12 * BS) ** -0.5, 0.15625, ((0, 2),)),
        "coupling": gaussian(streams_of[3], (2 * F,), 0.5, 3.0, ((0, 64),), jnp.float32),
        "frequencies": jnp.clip(jax.random.uniform(streams_of[4], (F,), jnp.float32, 1.0, 1024.0), 1.0, 1024.0),
        "receivers": touch_ends(jax.random.randint(streams_of[5], (R,), 0, NZ), jax.random.fold_in(streams_of[5], 1), 0, NZ - 1).astype(jnp.int32),
        "floors": touch_ends(jax.random.randint(streams_of[6], (STEPS,), NZ // 4, NZ), jax.random.fold_in(streams_of[6], 1), NZ // 4, NZ - 1).astype(jnp.int32),
    }


def apply_blocks(blocks, padded):
    block_count = blocks.shape[0]
    width = padded.shape[1]
    stacked = padded.reshape(block_count + 2, BS, width)
    neighbours = jnp.stack([stacked[:-2], stacked[1:-1], stacked[2:]], axis=1)
    product = jnp.einsum('bikrj,bkjc->rbic', blocks, neighbours, precision=lax.Precision.HIGHEST)
    real_part = product[0].reshape(block_count * BS, width)
    imag_part = product[1].reshape(block_count * BS, width // 2, 2)
    rotated = jnp.stack([-imag_part[..., 1], imag_part[..., 0]], axis=-1).reshape(block_count * BS, width)
    return real_part + rotated

def couple_terms(values, weights):
    height = values.shape[0]
    paired = values.reshape(height, -1, 2)
    wpair = weights.reshape(-1, 2)
    real_part = wpair[:, 0] * paired[..., 0] - wpair[:, 1] * paired[..., 1]
    imag_part = wpair[:, 0] * paired[..., 1] + wpair[:, 1] * paired[..., 0]
    return jnp.stack([real_part, imag_part], axis=-1).reshape(height, -1)

def make_basis(freq_values, sample_times):
    phase = jnp.mod(freq_values[:, None] * sample_times[None, :], jnp.float32(NT)) / jnp.float32(NT)
    angle = 2.0 * math.pi * phase
    stacked = jnp.stack([jnp.cos(angle), -jnp.sin(angle)], axis=1)
    return stacked.reshape(2 * freq_values.shape[0], sample_times.shape[0]).astype(jnp.bfloat16)

def reference(pressure_field, block_main, block_coupled, coupling, frequencies, receivers, floors):
    block_count = NZ // BS
    main_blocks = block_main.astype(jnp.float32).reshape(block_count, BS, 3, 2, BS)
    side_blocks = block_coupled.astype(jnp.float32).reshape(block_count, BS, 3, 2, BS)
    grouped = pressure_field.reshape(NZ, N_FREQ, 2 * F_DEV).transpose(1, 0, 2)
    pairs = coupling.reshape(N_FREQ, 2 * F_DEV)
    freq_groups = frequencies.reshape(N_FREQ, F_DEV)
    depth_index = jnp.arange(NZ, dtype=jnp.int32)
    sample_times = jnp.arange(NT, dtype=jnp.float32)

    def one_group(running, group_items):
        columns, weights, freq_values = group_items
        for step in range(STEPS):
            padded = jnp.pad(columns.astype(jnp.float32), ((BS, BS), (0, 0)))
            combined = apply_blocks(main_blocks, padded) + couple_terms(apply_blocks(side_blocks, padded), weights)
            damping = jnp.where(depth_index >= floors[step], 0.5, 1.0).astype(jnp.float32)
            columns = (damping[:, None] * combined).astype(jnp.bfloat16)
        picked = jnp.take(columns, receivers, axis=0)
        basis_table = make_basis(freq_values, sample_times)
        return (running + jnp.dot(picked, basis_table, preferred_element_type=jnp.float32), None)
    running, _ = lax.scan(one_group, jnp.zeros((R, NT), jnp.float32), (grouped, pairs, freq_groups))
    return running * (1.0 / math.sqrt(F))
```

```python
import functools
import math

import jax
import jax.numpy as jnp
from jax import lax
from jax.experimental import pallas as pl
from jax.experimental.pallas import tpu as pltpu
from jax.sharding import PartitionSpec as P

NT = 2048
STEPS = 4
BS = 128
MESH = pl.DeviceIdType.MESH
F32 = jnp.float32
BF16 = jnp.bfloat16


def iota(shape, dim):
    return lax.broadcasted_iota(jnp.int32, shape, dim)


def dot(a, b):
    return jnp.dot(a, b, preferred_element_type=F32)


def dot_nt(a, b):
    return lax.dot_general(a, b, (((1,), (1,)), ((), ())), preferred_element_type=F32)


def times_unit(x):
    return jnp.concatenate([-x[:, BS:], x[:, :BS]], axis=1)


def march_kernel(
    nb,
    unroll,
    field_hbm,
    main_hbm,
    side_hbm,
    coupling,
    receivers,
    floors,
    picked_out,
    raw_field,
    raw_main,
    raw_side,
    ops,
    state,
    final,
    selector,
    recv_col,
    weights,
    split,
    order,
    halo,
    theirs,
    arrived,
    field_sem,
    main_sem,
    side_sem,
    halo_send,
    halo_recv,
    pick_send,
    pick_recv,
):
    depth = lax.axis_index("depth")
    other = 1 - depth
    width = 2 * BS
    rows_here = nb * BS
    first_row = depth * rows_here
    half = theirs.shape[0]

    def block_at(i):
        return jnp.where(depth == 0, i, nb - 1 - i)

    edge = block_at(nb - 1)
    halo_slot = jnp.where(depth == 0, nb + 1, 0)

    def field_copy(b):
        return pltpu.make_async_copy(
            field_hbm.at[pl.ds(pl.multiple_of(b * BS, BS), BS), :],
            raw_field.at[pl.ds(pl.multiple_of(b * BS, BS), BS), :],
            field_sem.at[b],
        )

    def op_copy(hbm, raw, sem, b):
        rows = 6 * BS
        return pltpu.make_async_copy(
            hbm.at[pl.ds(pl.multiple_of(b * rows, rows), rows), :],
            raw.at[pl.ds(pl.multiple_of(b * rows, rows), rows), :],
            sem.at[b],
        )

    field_copy(edge).start()

    @pl.loop(0, nb - 1)
    def _(i):
        field_copy(block_at(i)).start()

    @pl.loop(0, nb)
    def _(i):
        op_copy(main_hbm, raw_main, main_sem, block_at(i)).start()
        op_copy(side_hbm, raw_side, side_sem, block_at(i)).start()

    barrier = pltpu.get_barrier_semaphore()
    pl.semaphore_signal(barrier, inc=1, device_id={"depth": other}, device_id_type=MESH)

    row, col = iota((width, width), 0), iota((width, width), 1)
    wanted = jnp.where(col < BS, 2 * col, 2 * (col - BS) + 1)
    split[...] = jnp.where(row == wanted, 1.0, 0.0).astype(BF16)
    row, col = iota((192, 192), 0), iota((192, 192), 1)
    order[...] = jnp.where(col == 6 * (row & 31) + (row >> 5), 1.0, 0.0).astype(BF16)
    split_f32 = split[...].astype(F32)
    weights[...] = jnp.dot(
        jnp.broadcast_to(coupling[...], (8, width)),
        split_f32,
        precision=lax.Precision.HIGHEST,
        preferred_element_type=F32,
    )
    spots = receivers[...].astype(F32)
    for g in range(receivers.shape[0]):
        tile = jnp.broadcast_to(spots[g : g + 1, :], (BS, BS))
        recv_col[g * BS : (g + 1) * BS, :] = tile.T
    empty = jnp.zeros((2 * BS, width), BF16)
    for par in range(2):
        state[par, 0 : 2 * BS, :] = empty
        state[par, (nb + 1) * 2 * BS : (nb + 2) * 2 * BS, :] = empty

    def put(par, slot, x):
        start = pl.multiple_of(slot * 2 * BS, 2 * BS)
        state[par, pl.ds(start, BS), :] = x
        state[par, pl.ds(start + BS, BS), :] = times_unit(x)

    def halo_copy(step, src):
        return pltpu.make_async_remote_copy(
            src_ref=src,
            dst_ref=halo.at[step],
            send_sem=halo_send.at[step],
            recv_sem=halo_recv.at[step],
            device_id={"depth": other},
            device_id_type=MESH,
        )

    field_copy(edge).wait()
    pl.semaphore_wait(barrier, 1)
    edge_rows = pl.ds(pl.multiple_of(edge * BS, BS), BS)
    first_halo = halo_copy(0, raw_field.at[edge_rows, :])
    first_halo.start()

    def deinterleave(b):
        rows = pl.ds(pl.multiple_of(b * BS, BS), BS)
        put(0, b + 1, dot(raw_field[rows, :], split[...]).astype(BF16))

    @pl.loop(0, (nb - unroll) // unroll)
    def _(t):
        for u in range(unroll):
            field_copy(block_at(t * unroll + u)).wait()
        for u in range(unroll):
            deinterleave(block_at(t * unroll + u))

    for u in range(unroll - 1):
        field_copy(block_at(nb - unroll + u)).wait()
    for u in range(unroll):
        deinterleave(block_at(nb - unroll + u))

    def bring_in(b):
        base = pl.multiple_of(b * 6 * BS, 6 * BS)
        dest = pl.multiple_of(b * 2 * BS, 2 * BS)
        for q in range(4):
            part = pl.ds(base + 192 * q, 192)
            both = jnp.concatenate([raw_main[part, :], raw_side[part, :]], axis=1)
            sorted_rows = dot(order[...], both).astype(BF16)
            for kc in range(6):
                tile = sorted_rows[32 * kc : 32 * kc + 32, :]
                lanes = slice(kc * BS, (kc + 1) * BS)
                ops[pl.ds(dest + 32 * q, 32), lanes] = tile[:, :BS]
                ops[pl.ds(dest + BS + 32 * q, 32), lanes] = tile[:, BS:]

    def select(b):
        target = (first_row + b * BS).astype(F32)
        lane = iota((2 * half, BS), 1).astype(F32) + target
        lanes = pl.ds(pl.multiple_of(b * BS, BS), BS)
        selector[:, lanes] = jnp.where(recv_col[...] == lane, 1.0, 0.0).astype(BF16)

    def advance(step, par, b):
        lhs = ops[pl.ds(pl.multiple_of(b * 2 * BS, 2 * BS), 2 * BS), :]
        rhs = state[par, pl.ds(pl.multiple_of(b * 2 * BS, 2 * BS), 6 * BS), :]
        product = dot(lhs, rhs)
        main, side = product[:BS], product[BS:]
        w_real, w_imag = weights[0:1, :BS], weights[0:1, BS:]
        side_real, side_imag = side[:, :BS], side[:, BS:]
        real = main[:, :BS] + (w_real * side_real - w_imag * side_imag)
        imag = main[:, BS:] + (w_real * side_imag + w_imag * side_real)
        depth_index = first_row + b * BS + iota((BS, BS), 0)
        damping = jnp.where(depth_index >= floors[step], 0.5, 1.0).astype(F32)
        return jnp.concatenate([damping * real, damping * imag], axis=1).astype(BF16)

    trips = nb // unroll

    @pl.loop(0, trips)
    def _(t):
        @pl.when(t == trips - 1)
        def _():
            first_halo.wait()
            put(0, halo_slot, dot(halo[0], split[...]).astype(BF16))

        for u in range(unroll):
            b = block_at(t * unroll + u)
            op_copy(main_hbm, raw_main, main_sem, b).wait()
            op_copy(side_hbm, raw_side, side_sem, b).wait()
        for u in range(unroll):
            b = block_at(t * unroll + u)
            bring_in(b)
            select(b)
        for u in range(unroll):
            b = block_at(t * unroll + u)
            put(1, b + 1, advance(0, 0, b))

    def edge_of(par):
        return state.at[par, pl.ds(pl.multiple_of((edge + 1) * 2 * BS, 2 * BS), BS), :]

    halo_copy(1, edge_of(1)).start()

    @pl.loop(1, STEPS - 1)
    def _(step):
        par = step & 1

        @pl.loop(0, trips)
        def _(t):
            @pl.when(t == trips - 1)
            def _():
                halo_copy(step, edge_of(par)).wait()
                put(par, halo_slot, halo[step])

            for u in range(unroll):
                b = block_at(t * unroll + u)
                put(1 - par, b + 1, advance(step, par, b))

        halo_copy(step + 1, edge_of(1 - par)).start()

    par = (STEPS - 1) & 1

    @pl.loop(0, trips)
    def _(t):
        @pl.when(t == trips - 1)
        def _():
            halo_copy(STEPS - 1, edge_of(par)).wait()
            put(par, halo_slot, halo[STEPS - 1])

        for u in range(unroll):
            b = block_at(t * unroll + u)
            final[pl.ds(pl.multiple_of(b * BS, BS), BS), :] = advance(STEPS - 1, par, b)

    def pick(owner):
        rows = pl.ds(pl.multiple_of(owner * half, half), half)
        return dot(selector[rows, :], final[...]).astype(BF16)

    theirs[...] = pick(other)
    swap = pltpu.make_async_remote_copy(
        src_ref=theirs,
        dst_ref=arrived,
        send_sem=pick_send,
        recv_sem=pick_recv,
        device_id={"depth": other},
        device_id_type=MESH,
    )
    swap.start()
    mine = pick(depth)
    swap.wait()
    picked_out[...] = mine + arrived[...]


def poly_coeffs():
    import numpy as np

    x = np.cos(np.pi * (np.arange(400) + 0.5) / 400) * 0.125 + 0.125
    y = np.sqrt(x)
    cheb_c = np.polynomial.chebyshev.Chebyshev.fit(x, np.cos(2 * np.pi * y), 8, domain=[0, 0.25])
    cheb_s = np.polynomial.chebyshev.Chebyshev.fit(x, np.sin(2 * np.pi * y) / y, 8, domain=[0, 0.25])
    to = np.polynomial.polynomial.Polynomial
    return (
        [float(v) for v in cheb_c.convert(kind=to).coef],
        [float(v) for v in cheb_s.convert(kind=to).coef],
    )


COS_COEFFS, SIN_COEFFS = poly_coeffs()


def horner(coeffs, z):
    total = jnp.full_like(z, coeffs[-1])
    for c in reversed(coeffs[:-1]):
        total = total * z + c
    return total


def cos_sin(turns):
    r = turns - jnp.floor(turns + 0.5)
    z = r * r
    return horner(COS_COEFFS, z), r * horner(SIN_COEFFS, z)


def synth_kernel(
    chips,
    factor,
    picked,
    frequencies,
    out,
    partner,
    basis,
    near,
    far,
    sums,
    inbox,
    pair_send,
    pair_recv,
    send_sem,
    recv_sem,
):
    me = lax.axis_index("freq")
    chip, core = me // 2, me % 2
    span = NT // (2 * chips)
    rows = picked.shape[0]

    barrier = pltpu.get_barrier_semaphore()
    mate = 2 * chip + (1 - core)
    pl.semaphore_signal(barrier, inc=1, device_id={"freq": mate}, device_id_type=MESH)

    @pl.loop(1, chips)
    def _(k):
        peer = 2 * ((chip + k) % chips) + core
        pl.semaphore_signal(barrier, inc=1, device_id={"freq": peer}, device_id_type=MESH)

    pl.semaphore_wait(barrier, chips)

    swap = pltpu.make_async_remote_copy(
        src_ref=picked,
        dst_ref=partner,
        send_sem=pair_send,
        recv_sem=pair_recv,
        device_id={"freq": mate},
        device_id_type=MESH,
    )
    swap.start()

    own_f = frequencies[pl.ds(me, 1), :]
    mate_f = frequencies[pl.ds(mate, 1), :]
    freq = jnp.concatenate([own_f, mate_f], axis=1)
    scale = 1.0 / NT
    step_in = iota((span, 2 * BS), 0).astype(F32)
    cos_b, sin_b = cos_sin(freq * step_in * scale)
    start = ((2 * iota((chips, 2 * BS), 0) + core) * span).astype(F32)
    cos_a, sin_a = cos_sin(freq * start * scale)
    near[0], near[1] = cos_b, sin_b
    far[0], far[1] = cos_a, sin_a

    @pl.loop(0, chips)
    def _(j):
        ca, sa = far[0, pl.ds(j, 1), :], far[1, pl.ds(j, 1), :]
        cb, sb = near[0], near[1]
        real = (ca * cb - sa * sb).astype(BF16)
        imag = (-(sa * cb + ca * sb)).astype(BF16)
        place = pl.ds(pl.multiple_of(j * span, span), span)
        basis[place, 0:BS] = real[:, :BS]
        basis[place, BS : 2 * BS] = imag[:, :BS]
        basis[place, 2 * BS : 3 * BS] = real[:, BS:]
        basis[place, 3 * BS : 4 * BS] = imag[:, BS:]

    swap.wait()

    def outgoing(j):
        return pltpu.make_async_remote_copy(
            src_ref=sums.at[j],
            dst_ref=inbox.at[chip],
            send_sem=send_sem.at[j],
            recv_sem=recv_sem.at[chip],
            device_id={"freq": 2 * j + core},
            device_id_type=MESH,
        )

    def incoming(j):
        return pltpu.make_async_remote_copy(
            src_ref=sums.at[chip],
            dst_ref=inbox.at[j],
            send_sem=send_sem.at[chip],
            recv_sem=recv_sem.at[j],
            device_id={"freq": 2 * j + core},
            device_id_type=MESH,
        )

    batch = min(8, chips)

    @pl.loop(0, chips // batch)
    def _(g):
        group = (chip // batch + g) % (chips // batch)
        place = pl.ds(pl.multiple_of(group * batch * span, batch * span), batch * span)
        part = dot_nt(basis[place, : 2 * BS], picked[...]) + dot_nt(
            basis[place, 2 * BS :], partner[...]
        )
        part = (part * factor).astype(BF16)
        for u in range(batch):
            sums[group * batch + u] = part[u * span : (u + 1) * span, :]
        for u in range(batch):
            j = group * batch + u

            @pl.when(j != chip)
            def _():
                outgoing(j).start()

    inbox[chip] = sums[chip]

    @pl.loop(1, chips)
    def _(k):
        incoming((chip + k) % chips).wait_recv()

    total = inbox[0].astype(F32)
    for j in range(1, chips):
        total = total + inbox[j].astype(F32)
    out[...] = total

    @pl.loop(1, chips)
    def _(k):
        outgoing((chip + k) % chips).wait_send()


def local(pressure_field, block_main, block_coupled, coupling, frequencies, receivers, floors):
    rows_here, width = pressure_field.shape
    nb = rows_here // BS
    unroll = min(8, nb // 2)
    count = receivers.shape[0]
    half = count // 2
    any_space = pl.BlockSpec(memory_space=pl.ANY)
    vmem = pl.BlockSpec(memory_space=pltpu.VMEM)
    smem = pl.BlockSpec(memory_space=pltpu.SMEM)
    dma = pltpu.SemaphoreType.DMA
    picked = pl.pallas_call(
        functools.partial(march_kernel, nb, unroll),
        out_shape=jax.ShapeDtypeStruct((half, width), BF16),
        in_specs=[any_space, any_space, any_space, vmem, vmem, smem],
        out_specs=vmem,
        scratch_shapes=[
            pltpu.VMEM((rows_here, width), BF16),
            pltpu.VMEM((rows_here * 6, BS), BF16),
            pltpu.VMEM((rows_here * 6, BS), BF16),
            pltpu.VMEM((nb * 2 * BS, 6 * BS), BF16),
            pltpu.VMEM((2, (nb + 2) * 2 * BS, width), BF16),
            pltpu.VMEM((rows_here, width), BF16),
            pltpu.VMEM((count, rows_here), BF16),
            pltpu.VMEM((count, BS), F32),
            pltpu.VMEM((8, width), F32),
            pltpu.VMEM((width, width), BF16),
            pltpu.VMEM((192, 192), BF16),
            pltpu.VMEM((STEPS, BS, width), BF16),
            pltpu.VMEM((half, width), BF16),
            pltpu.VMEM((half, width), BF16),
            dma((nb,)),
            dma((nb,)),
            dma((nb,)),
            dma((STEPS,)),
            dma((STEPS,)),
            dma,
            dma,
        ],
        compiler_params=pltpu.CompilerParams(
            collective_id=0, has_side_effects=True, vmem_limit_bytes=60 * 1024 * 1024
        ),
        name="march",
    )(
        pressure_field,
        block_main.reshape(rows_here * 6, BS),
        block_coupled.reshape(rows_here * 6, BS),
        coupling.reshape(1, width),
        receivers.reshape(count // BS, BS),
        floors,
    )
    chips = lax.axis_size("freq") // 2
    span = NT // (2 * chips)
    total_freq = frequencies.shape[0]
    summed = pl.pallas_call(
        functools.partial(synth_kernel, chips, 1.0 / math.sqrt(total_freq)),
        out_shape=jax.ShapeDtypeStruct((span, half), F32),
        in_specs=[vmem, vmem],
        out_specs=vmem,
        scratch_shapes=[
            pltpu.VMEM((half, width), BF16),
            pltpu.VMEM((NT // 2, 2 * width), BF16),
            pltpu.VMEM((2, span, width), F32),
            pltpu.VMEM((2, chips, width), F32),
            pltpu.VMEM((chips, span, half), BF16),
            pltpu.VMEM((chips, span, half), BF16),
            dma,
            dma,
            dma((chips,)),
            dma((chips,)),
        ],
        compiler_params=pltpu.CompilerParams(collective_id=1, has_side_effects=True),
        name="synth",
    )(picked, frequencies.reshape(total_freq // BS, BS))
    return summed.T


def solution(mesh):
    in_specs = (
        P("depth", "freq"),
        P("depth", None, None, None),
        P("depth", None, None, None),
        P("freq"),
        P(),
        P(),
        P(),
    )
    out_specs = P("depth", "freq")
    return jax.shard_map(local, mesh=mesh, in_specs=in_specs, out_specs=out_specs, check_vma=False)
```

```python
import functools
import math

import jax
import jax.numpy as jnp
from jax import lax
from jax.experimental import pallas as pl
from jax.experimental.pallas import tpu as pltpu
from jax.sharding import PartitionSpec as P

NT = 2048
STEPS = 4
BS = 128
MESH = pl.DeviceIdType.MESH
F32 = jnp.float32
BF16 = jnp.bfloat16


def iota(shape, dim):
    return lax.broadcasted_iota(jnp.int32, shape, dim)


def dot(a, b):
    return jnp.dot(a, b, preferred_element_type=F32)


def dot_nt(a, b):
    return lax.dot_general(a, b, (((1,), (1,)), ((), ())), preferred_element_type=F32)


def times_unit(x):
    return jnp.concatenate([-x[:, BS:], x[:, :BS]], axis=1)


def march_kernel(
    nb,
    unroll,
    field_hbm,
    main_hbm,
    side_hbm,
    coupling,
    receivers,
    floors,
    picked_out,
    raw_field,
    raw_main,
    raw_side,
    ops,
    state_a,
    state_b,
    final,
    selector,
    recv_col,
    weights,
    split,
    order,
    halo,
    theirs,
    arrived,
    field_sem,
    main_sem,
    side_sem,
    halo_send,
    halo_recv,
    pick_send,
    pick_recv,
):
    depth = lax.axis_index("depth")
    other = 1 - depth
    width = 2 * BS
    first_row = depth * nb * BS
    half = theirs.shape[0]
    trips = nb // unroll

    def block_at(i):
        return jnp.where(depth == 0, i, nb - 1 - i)

    def rows_of(i, count):
        return pl.ds(pl.multiple_of(i * count, count), count)

    def field_copy(i):
        return pltpu.make_async_copy(
            field_hbm.at[rows_of(block_at(i), BS), :],
            raw_field.at[rows_of(i, BS), :],
            field_sem.at[i],
        )

    def op_copy(hbm, raw, sem, i):
        return pltpu.make_async_copy(
            hbm.at[rows_of(block_at(i), 6 * BS), :], raw.at[rows_of(i, 6 * BS), :], sem.at[i]
        )

    field_copy(nb - 1).start()

    @pl.loop(0, nb - 1)
    def _(i):
        field_copy(i).start()

    @pl.loop(0, nb)
    def _(i):
        op_copy(main_hbm, raw_main, main_sem, i).start()
        op_copy(side_hbm, raw_side, side_sem, i).start()

    barrier = pltpu.get_barrier_semaphore()
    pl.semaphore_signal(barrier, inc=1, device_id={"depth": other}, device_id_type=MESH)

    row, col = iota((width, width), 0), iota((width, width), 1)
    wanted = jnp.where(col < BS, 2 * col, 2 * (col - BS) + 1)
    split[...] = jnp.where(row == wanted, 1.0, 0.0).astype(BF16)
    row, col = iota((192, 192), 0), iota((192, 192), 1)
    k, c, d = row >> 6, (row >> 5) & 1, row & 31
    k = jnp.where(depth == 0, k, 2 - k)
    order[...] = jnp.where(col == 6 * d + 2 * k + c, 1.0, 0.0).astype(BF16)
    weights[...] = jnp.dot(
        jnp.broadcast_to(coupling[...], (8, width)),
        split[...].astype(F32),
        precision=lax.Precision.HIGHEST,
        preferred_element_type=F32,
    )
    spots = receivers[...].astype(F32)
    for g in range(receivers.shape[0]):
        tile = jnp.broadcast_to(spots[g : g + 1, :], (BS, BS))
        recv_col[g * BS : (g + 1) * BS, :] = tile.T
    empty = jnp.zeros((2 * BS, width), BF16)
    for state in (state_a, state_b):
        state[0 : 2 * BS, :] = empty

    def put(state, slot, x):
        state[rows_of(2 * slot, BS), :] = x
        state[rows_of(2 * slot + 1, BS), :] = times_unit(x)

    def halo_copy(step, src):
        return pltpu.make_async_remote_copy(
            src_ref=src,
            dst_ref=halo.at[step],
            send_sem=halo_send.at[step],
            recv_sem=halo_recv.at[step],
            device_id={"depth": other},
            device_id_type=MESH,
        )

    field_copy(nb - 1).wait()
    pl.semaphore_wait(barrier, 1)
    first_halo = halo_copy(0, raw_field.at[rows_of(nb - 1, BS), :])
    first_halo.start()

    def deinterleave(i):
        put(state_a, i + 1, dot(raw_field[rows_of(i, BS), :], split[...]).astype(BF16))

    @pl.loop(0, nb - 1)
    def _(i):
        field_copy(i).wait()

    @pl.loop(0, trips)
    def _(t):
        for u in range(unroll):
            deinterleave(t * unroll + u)

    def bring_in(i):
        for q in range(4):
            part = pl.ds(pl.multiple_of(i * 6 * BS, 6 * BS) + 192 * q, 192)
            both = jnp.concatenate([raw_main[part, :], raw_side[part, :]], axis=1)
            sorted_rows = dot(order[...], both).astype(BF16)
            dest = pl.multiple_of(i * 2 * BS, 2 * BS) + 32 * q
            for kc in range(6):
                tile = sorted_rows[32 * kc : 32 * kc + 32, :]
                lanes = slice(kc * BS, (kc + 1) * BS)
                ops[pl.ds(dest, 32), lanes] = tile[:, :BS]
                ops[pl.ds(dest + BS, 32), lanes] = tile[:, BS:]

    def select(i):
        target = (first_row + block_at(i) * BS).astype(F32)
        lane = iota((2 * half, BS), 1).astype(F32) + target
        selector[:, rows_of(i, BS)] = jnp.where(recv_col[...] == lane, 1.0, 0.0).astype(BF16)

    def advance(step, state, i):
        product = dot(ops[rows_of(i, 2 * BS), :], state[pl.ds(pl.multiple_of(i * 2 * BS, 2 * BS), 6 * BS), :])
        main, side = product[:BS], product[BS:]
        w_real, w_imag = weights[0:1, :BS], weights[0:1, BS:]
        side_real, side_imag = side[:, :BS], side[:, BS:]
        real = main[:, :BS] + (w_real * side_real - w_imag * side_imag)
        imag = main[:, BS:] + (w_real * side_imag + w_imag * side_real)
        depth_index = first_row + block_at(i) * BS + iota((BS, BS), 0)
        damping = jnp.where(depth_index >= floors[step], 0.5, 1.0).astype(F32)
        return jnp.concatenate([damping * real, damping * imag], axis=1).astype(BF16)

    def wait_ops(t):
        for u in range(unroll):
            op_copy(main_hbm, raw_main, main_sem, t * unroll + u).wait()
            op_copy(side_hbm, raw_side, side_sem, t * unroll + u).wait()

    wait_ops(0)
    for u in range(unroll):
        bring_in(u)
        select(u)

    @pl.loop(1, trips)
    def _(t):
        wait_ops(t)
        for u in range(unroll):
            put(state_b, (t - 1) * unroll + u + 1, advance(0, state_a, (t - 1) * unroll + u))
            bring_in(t * unroll + u)
            select(t * unroll + u)

    first_halo.wait()
    put(state_a, nb + 1, dot(halo[0], split[...]).astype(BF16))
    for i in range(nb - unroll, nb):
        put(state_b, i + 1, advance(0, state_a, i))

    def edge_of(state):
        return state.at[rows_of(2 * nb, BS), :]

    states = (state_a, state_b)
    for step in range(1, STEPS):
        now, later = states[step % 2], states[1 - step % 2]
        arrival = halo_copy(step, edge_of(now))
        arrival.start()

        def go(i):
            x = advance(step, now, i)
            if step < STEPS - 1:
                put(later, i + 1, x)
            else:
                final[rows_of(i, BS), :] = x

        for i in range(nb - unroll):
            go(i)
        arrival.wait()
        put(now, nb + 1, halo[step])
        for i in range(nb - unroll, nb):
            go(i)

    def pick(owner):
        parts = []
        for p in range(2):
            rows = pl.ds(pl.multiple_of(owner * half, half) + p * (half // 2), half // 2)
            parts.append(dot(selector[rows, :], final[...]).astype(BF16))
        return jnp.concatenate(parts, axis=0)

    theirs[...] = pick(other)
    swap = pltpu.make_async_remote_copy(
        src_ref=theirs,
        dst_ref=arrived,
        send_sem=pick_send,
        recv_sem=pick_recv,
        device_id={"depth": other},
        device_id_type=MESH,
    )
    swap.start()
    mine = pick(depth)
    swap.wait()
    picked_out[...] = mine + arrived[...]


def poly_coeffs():
    import numpy as np

    x = np.cos(np.pi * (np.arange(400) + 0.5) / 400) * 0.125 + 0.125
    y = np.sqrt(x)
    cheb_c = np.polynomial.chebyshev.Chebyshev.fit(x, np.cos(2 * np.pi * y), 8, domain=[0, 0.25])
    cheb_s = np.polynomial.chebyshev.Chebyshev.fit(x, np.sin(2 * np.pi * y) / y, 8, domain=[0, 0.25])
    to = np.polynomial.polynomial.Polynomial
    return (
        [float(v) for v in cheb_c.convert(kind=to).coef],
        [float(v) for v in cheb_s.convert(kind=to).coef],
    )


COS_COEFFS, SIN_COEFFS = poly_coeffs()


def horner(coeffs, z):
    total = jnp.full_like(z, coeffs[-1])
    for c in reversed(coeffs[:-1]):
        total = total * z + c
    return total


def cos_sin(turns):
    r = turns - jnp.floor(turns + 0.5)
    z = r * r
    return horner(COS_COEFFS, z), r * horner(SIN_COEFFS, z)


def synth_kernel(
    chips,
    factor,
    picked,
    frequencies,
    out,
    partner,
    basis,
    near,
    far,
    sums,
    inbox,
    pair_send,
    pair_recv,
    send_sem,
    recv_sem,
):
    me = lax.axis_index("freq")
    chip, core = me // 2, me % 2
    span = NT // (2 * chips)
    rows = picked.shape[0]

    barrier = pltpu.get_barrier_semaphore()
    mate = 2 * chip + (1 - core)
    pl.semaphore_signal(barrier, inc=1, device_id={"freq": mate}, device_id_type=MESH)

    @pl.loop(1, chips)
    def _(k):
        peer = 2 * ((chip + k) % chips) + core
        pl.semaphore_signal(barrier, inc=1, device_id={"freq": peer}, device_id_type=MESH)

    pl.semaphore_wait(barrier, chips)

    swap = pltpu.make_async_remote_copy(
        src_ref=picked,
        dst_ref=partner,
        send_sem=pair_send,
        recv_sem=pair_recv,
        device_id={"freq": mate},
        device_id_type=MESH,
    )
    swap.start()

    own_f = frequencies[pl.ds(me, 1), :]
    mate_f = frequencies[pl.ds(mate, 1), :]
    freq = jnp.concatenate([own_f, mate_f], axis=1)
    scale = 1.0 / NT
    step_in = iota((span, 2 * BS), 0).astype(F32)
    cos_b, sin_b = cos_sin(freq * step_in * scale)
    start = ((2 * iota((chips, 2 * BS), 0) + core) * span).astype(F32)
    cos_a, sin_a = cos_sin(freq * start * scale)
    near[0], near[1] = cos_b, sin_b
    far[0], far[1] = cos_a, sin_a

    @pl.loop(0, chips)
    def _(j):
        ca, sa = far[0, pl.ds(j, 1), :], far[1, pl.ds(j, 1), :]
        cb, sb = near[0], near[1]
        real = (ca * cb - sa * sb).astype(BF16)
        imag = (-(sa * cb + ca * sb)).astype(BF16)
        place = pl.ds(pl.multiple_of(j * span, span), span)
        basis[place, 0:BS] = real[:, :BS]
        basis[place, BS : 2 * BS] = imag[:, :BS]
        basis[place, 2 * BS : 3 * BS] = real[:, BS:]
        basis[place, 3 * BS : 4 * BS] = imag[:, BS:]

    swap.wait()

    def outgoing(j):
        return pltpu.make_async_remote_copy(
            src_ref=sums.at[j],
            dst_ref=inbox.at[chip],
            send_sem=send_sem.at[j],
            recv_sem=recv_sem.at[chip],
            device_id={"freq": 2 * j + core},
            device_id_type=MESH,
        )

    def incoming(j):
        return pltpu.make_async_remote_copy(
            src_ref=sums.at[chip],
            dst_ref=inbox.at[j],
            send_sem=send_sem.at[chip],
            recv_sem=recv_sem.at[j],
            device_id={"freq": 2 * j + core},
            device_id_type=MESH,
        )

    batch = min(8, chips)

    @pl.loop(0, chips // batch)
    def _(g):
        group = (chip // batch + g) % (chips // batch)
        place = pl.ds(pl.multiple_of(group * batch * span, batch * span), batch * span)
        part = dot_nt(basis[place, : 2 * BS], picked[...]) + dot_nt(
            basis[place, 2 * BS :], partner[...]
        )
        part = (part * factor).astype(BF16)
        for u in range(batch):
            sums[group * batch + u] = part[u * span : (u + 1) * span, :]
        for u in range(batch):
            j = group * batch + u

            @pl.when(j != chip)
            def _():
                outgoing(j).start()

    inbox[chip] = sums[chip]

    @pl.loop(1, chips)
    def _(k):
        incoming((chip + k) % chips).wait_recv()

    total = inbox[0].astype(F32)
    for j in range(1, chips):
        total = total + inbox[j].astype(F32)
    out[...] = total

    @pl.loop(1, chips)
    def _(k):
        outgoing((chip + k) % chips).wait_send()


def local(pressure_field, block_main, block_coupled, coupling, frequencies, receivers, floors):
    rows_here, width = pressure_field.shape
    nb = rows_here // BS
    unroll = min(8, nb // 2)
    count = receivers.shape[0]
    half = count // 2
    any_space = pl.BlockSpec(memory_space=pl.ANY)
    vmem = pl.BlockSpec(memory_space=pltpu.VMEM)
    smem = pl.BlockSpec(memory_space=pltpu.SMEM)
    dma = pltpu.SemaphoreType.DMA
    picked = pl.pallas_call(
        functools.partial(march_kernel, nb, unroll),
        out_shape=jax.ShapeDtypeStruct((half, width), BF16),
        in_specs=[any_space, any_space, any_space, vmem, vmem, smem],
        out_specs=vmem,
        scratch_shapes=[
            pltpu.VMEM((rows_here, width), BF16),
            pltpu.VMEM((rows_here * 6, BS), BF16),
            pltpu.VMEM((rows_here * 6, BS), BF16),
            pltpu.VMEM((nb * 2 * BS, 6 * BS), BF16),
            pltpu.VMEM(((nb + 2) * 2 * BS, width), BF16),
            pltpu.VMEM(((nb + 2) * 2 * BS, width), BF16),
            pltpu.VMEM((rows_here, width), BF16),
            pltpu.VMEM((count, rows_here), BF16),
            pltpu.VMEM((count, BS), F32),
            pltpu.VMEM((8, width), F32),
            pltpu.VMEM((width, width), BF16),
            pltpu.VMEM((192, 192), BF16),
            pltpu.VMEM((STEPS, BS, width), BF16),
            pltpu.VMEM((half, width), BF16),
            pltpu.VMEM((half, width), BF16),
            dma((nb,)),
            dma((nb,)),
            dma((nb,)),
            dma((STEPS,)),
            dma((STEPS,)),
            dma,
            dma,
        ],
        compiler_params=pltpu.CompilerParams(
            collective_id=0, has_side_effects=True, vmem_limit_bytes=60 * 1024 * 1024
        ),
        name="march",
    )(
        pressure_field,
        block_main.reshape(rows_here * 6, BS),
        block_coupled.reshape(rows_here * 6, BS),
        coupling.reshape(1, width),
        receivers.reshape(count // BS, BS),
        floors,
    )
    chips = lax.axis_size("freq") // 2
    span = NT // (2 * chips)
    total_freq = frequencies.shape[0]
    summed = pl.pallas_call(
        functools.partial(synth_kernel, chips, 1.0 / math.sqrt(total_freq)),
        out_shape=jax.ShapeDtypeStruct((span, half), F32),
        in_specs=[vmem, vmem],
        out_specs=vmem,
        scratch_shapes=[
            pltpu.VMEM((half, width), BF16),
            pltpu.VMEM((NT // 2, 2 * width), BF16),
            pltpu.VMEM((2, span, width), F32),
            pltpu.VMEM((2, chips, width), F32),
            pltpu.VMEM((chips, span, half), BF16),
            pltpu.VMEM((chips, span, half), BF16),
            dma,
            dma,
            dma((chips,)),
            dma((chips,)),
        ],
        compiler_params=pltpu.CompilerParams(collective_id=1, has_side_effects=True),
        name="synth",
    )(picked, frequencies.reshape(total_freq // BS, BS))
    return summed.T


def solution(mesh):
    in_specs = (
        P("depth", "freq"),
        P("depth", None, None, None),
        P("depth", None, None, None),
        P("freq"),
        P(),
        P(),
        P(),
    )
    out_specs = P("depth", "freq")
    return jax.shard_map(local, mesh=mesh, in_specs=in_specs, out_specs=out_specs, check_vma=False)
```

```python
import functools
import math

import jax
import jax.numpy as jnp
from jax import lax
from jax.experimental import pallas as pl
from jax.experimental.pallas import tpu as pltpu
from jax.sharding import PartitionSpec as P

NT = 2048
STEPS = 4
BS = 128
MESH = pl.DeviceIdType.MESH
F32 = jnp.float32
BF16 = jnp.bfloat16


def iota(shape, dim):
    return lax.broadcasted_iota(jnp.int32, shape, dim)


def dot(a, b):
    return jnp.dot(a, b, preferred_element_type=F32)


def dot_nt(a, b):
    return lax.dot_general(a, b, (((1,), (1,)), ((), ())), preferred_element_type=F32)


def poly_coeffs():
    import numpy as np

    x = np.cos(np.pi * (np.arange(400) + 0.5) / 400) * 0.125 + 0.125
    y = np.sqrt(x)
    cheb_c = np.polynomial.chebyshev.Chebyshev.fit(x, np.cos(2 * np.pi * y), 8, domain=[0, 0.25])
    cheb_s = np.polynomial.chebyshev.Chebyshev.fit(x, np.sin(2 * np.pi * y) / y, 8, domain=[0, 0.25])
    to = np.polynomial.polynomial.Polynomial
    return (
        [float(v) for v in cheb_c.convert(kind=to).coef],
        [float(v) for v in cheb_s.convert(kind=to).coef],
    )


COS_COEFFS, SIN_COEFFS = poly_coeffs()


def horner(coeffs, z):
    total = jnp.full_like(z, coeffs[-1])
    for c in reversed(coeffs[:-1]):
        total = total * z + c
    return total


def cos_sin(turns):
    r = turns - jnp.floor(turns + 0.5)
    z = r * r
    return horner(COS_COEFFS, z), r * horner(SIN_COEFFS, z)


def torus_offsets(chips):
    if chips != 32:
        return None
    found = []
    for dx in range(4):
        for dy in range(4):
            for dh in range(2):
                if dx or dy or dh:
                    found.append((min(dx, 4 - dx) + min(dy, 4 - dy) + 2 * dh, dx, dy, dh))
    return [entry[1:] for entry in sorted(found, key=lambda entry: (-entry[0],) + entry[1:])]


def peers_of(chip, chips, sign):
    offsets = torus_offsets(chips)
    if offsets is None:
        return [(chip + sign * k + chips) % chips for k in range(1, chips)]
    x, y, h = chip // 8, (chip // 2) % 4, chip % 2
    return [
        (((x + sign * dx + 4) % 4) * 4 + (y + sign * dy + 4) % 4) * 2 + (h + dh) % 2
        for dx, dy, dh in offsets
    ]


def kernel(
    nb,
    unroll,
    chips,
    factor,
    field_hbm,
    main_hbm,
    side_hbm,
    coupling_hbm,
    frequencies_hbm,
    receivers_hbm,
    floors,
    out,
    raw_field,
    raw_main,
    raw_side,
    ops,
    state_a,
    state_b,
    final_real,
    final_imag,
    selector,
    recv_col,
    weights,
    split,
    order,
    first_halo,
    halo,
    theirs,
    arrived,
    own,
    mate,
    basis,
    near,
    far,
    sums,
    inbox,
    coupling,
    frequencies,
    receivers,
    field_sem,
    main_sem,
    side_sem,
    small_sem,
    halo_send,
    halo_recv,
    swap_send,
    swap_recv,
    pair_send,
    pair_recv,
    out_send,
    out_recv,
):
    depth, me = lax.axis_index("depth"), lax.axis_index("freq")
    other = 1 - depth
    chip, core = me // 2, me % 2
    mate_id = 2 * chip + (1 - core)
    width = 2 * BS
    first_row = depth * nb * BS
    half = 2 * BS
    trips = nb // unroll
    span = NT // (2 * chips)

    def block_at(i):
        return jnp.where(depth == 0, i, nb - 1 - i)

    def rows_of(i, count):
        return pl.ds(pl.multiple_of(i * count, count), count)

    def field_copy(i):
        return pltpu.make_async_copy(
            field_hbm.at[rows_of(block_at(i), BS), :],
            raw_field.at[rows_of(i, BS), :],
            field_sem.at[i],
        )

    def op_copy(hbm, raw, sem, i):
        return pltpu.make_async_copy(
            hbm.at[rows_of(block_at(i), 6 * BS), :], raw.at[rows_of(i, 6 * BS), :], sem.at[i]
        )

    small = [
        pltpu.make_async_copy(coupling_hbm, coupling, small_sem.at[0]),
        pltpu.make_async_copy(receivers_hbm, receivers, small_sem.at[1]),
        pltpu.make_async_copy(frequencies_hbm, frequencies, small_sem.at[2]),
    ]
    for copy in small:
        copy.start()
    field_copy(nb - 1).start()

    @pl.loop(0, nb - 1)
    def _(i):
        field_copy(i).start()

    @pl.loop(0, nb)
    def _(i):
        op_copy(main_hbm, raw_main, main_sem, i).start()
        op_copy(side_hbm, raw_side, side_sem, i).start()

    barrier = pltpu.get_barrier_semaphore()

    def greet(target):
        pl.semaphore_signal(barrier, inc=1, device_id=target, device_id_type=MESH)

    greet({"depth": other})
    greet({"freq": mate_id})

    @pl.loop(1, chips)
    def _(k):
        greet({"freq": 2 * ((chip + k) % chips) + core})

    row, col = iota((width, width), 0), iota((width, width), 1)
    wanted = jnp.where(col < BS, 2 * col, 2 * (col - BS) + 1)
    split[...] = jnp.where(row == wanted, 1.0, 0.0).astype(BF16)
    row, col = iota((192, 192), 0), iota((192, 192), 1)
    k, c, d = row >> 6, (row >> 5) & 1, row & 31
    k = jnp.where(depth == 0, k, 2 - k)
    order[...] = jnp.where(col == 6 * d + 2 * k + c, 1.0, 0.0).astype(BF16)
    empty = jnp.zeros((3 * BS, BS), BF16)
    state_a[0 : 3 * BS, :] = empty
    state_b[0 : 3 * BS, :] = empty
    for copy in small:
        copy.wait()
    weights[...] = jnp.dot(
        jnp.broadcast_to(coupling[...], (8, width)),
        split[...].astype(F32),
        precision=lax.Precision.HIGHEST,
        preferred_element_type=F32,
    )
    spots = receivers[...].astype(F32)
    for g in range(receivers.shape[0]):
        tile = jnp.broadcast_to(spots[g : g + 1, :], (BS, BS))
        recv_col[g * BS : (g + 1) * BS, :] = tile.T

    freq = jnp.concatenate([frequencies[pl.ds(me, 1), :], frequencies[pl.ds(mate_id, 1), :]], axis=1)
    scale = 1.0 / NT
    near_n = iota((span, width), 0).astype(F32)
    near[0], near[1] = cos_sin(freq * near_n * scale)
    far_n = ((2 * iota((chips, width), 0) + core) * span).astype(F32)
    far[0], far[1] = cos_sin(freq * far_n * scale)

    def make_basis(j):
        ca, sa = far[0, j : j + 1, :], far[1, j : j + 1, :]
        cb, sb = near[0], near[1]
        real = (ca * cb - sa * sb).astype(BF16)
        imag = (-(sa * cb + ca * sb)).astype(BF16)
        for q, part in enumerate((real[:, :BS], imag[:, :BS], real[:, BS:], imag[:, BS:])):
            basis[q, j * span : (j + 1) * span, :] = part

    def put(state, slot, real, imag):
        state[rows_of(3 * slot, BS), :] = real
        state[rows_of(3 * slot + 1, BS), :] = imag
        state[rows_of(3 * slot + 2, BS), :] = -imag

    def remote(src, dst, send, recv, target):
        return pltpu.make_async_remote_copy(
            src_ref=src,
            dst_ref=dst,
            send_sem=send,
            recv_sem=recv,
            device_id=target,
            device_id_type=MESH,
        )

    def put_raw(slot, block):
        x = dot(block, split[...]).astype(BF16)
        put(state_a, slot, x[:, :BS], x[:, BS:])

    @pl.loop(0, nb)
    def _(i):
        field_copy(i).wait()

    @pl.loop(0, trips)
    def _(t):
        for u in range(unroll):
            put_raw(t * unroll + u + 1, raw_field[rows_of(t * unroll + u, BS), :])

    def bring_in(i):
        for q in range(4):
            part = pl.ds(pl.multiple_of(i * 6 * BS, 6 * BS) + 192 * q, 192)
            both = jnp.concatenate([raw_main[part, :], raw_side[part, :]], axis=1)
            sorted_rows = dot(order[...], both).astype(BF16)
            for kc in range(6):
                tile = sorted_rows[32 * kc : 32 * kc + 32, :]
                dest = pl.multiple_of(i * 12 * BS, 12 * BS) + kc * 2 * BS + 32 * q
                ops[pl.ds(dest, 32), :] = tile[:, :BS]
                ops[pl.ds(dest + BS, 32), :] = tile[:, BS:]

    def select(i):
        target = (first_row + block_at(i) * BS).astype(F32)
        lane = iota((2 * half, BS), 1).astype(F32) + target
        selector[rows_of(i, 2 * half), :] = jnp.where(recv_col[...] == lane, 1.0, 0.0).astype(BF16)

    def advance(step, state, i):
        lhs = jnp.concatenate([ops[rows_of(6 * i + kc, 2 * BS), :] for kc in range(6)], axis=1)
        tiles = []
        for slot in (i, i + 1, i + 2):
            real, imag, minus = (state[rows_of(3 * slot + q, BS), :] for q in range(3))
            tiles.append(jnp.concatenate([real, imag], axis=1))
            tiles.append(jnp.concatenate([minus, real], axis=1))
        product = dot(lhs, jnp.concatenate(tiles, axis=0))
        main, side = product[:BS], product[BS:]
        w_real, w_imag = weights[0:1, :BS], weights[0:1, BS:]
        side_real, side_imag = side[:, :BS], side[:, BS:]
        real = main[:, :BS] + (w_real * side_real - w_imag * side_imag)
        imag = main[:, BS:] + (w_real * side_imag + w_imag * side_real)
        depth_index = first_row + block_at(i) * BS + iota((BS, BS), 0)
        damping = jnp.where(depth_index >= floors[step], 0.5, 1.0).astype(F32)
        return (damping * real).astype(BF16), (damping * imag).astype(BF16)

    def load_group(t):
        for u in range(unroll):
            op_copy(main_hbm, raw_main, main_sem, t * unroll + u).wait()
            op_copy(side_hbm, raw_side, side_sem, t * unroll + u).wait()

    def first_step(i):
        put(state_b, i + 1, *advance(0, state_a, i))

    def pipelined(t):
        load_group(t)
        for u in range(unroll):
            first_step((t - 1) * unroll + u)
            bring_in(t * unroll + u)
            select(t * unroll + u)

    load_group(0)
    for u in range(unroll):
        bring_in(u)
        select(u)
    pipelined(1)
    pl.semaphore_wait(barrier, chips + 1)
    start_halo = remote(
        raw_field.at[rows_of(nb - 1, BS), :],
        first_halo,
        halo_send.at[0],
        halo_recv.at[0],
        {"depth": other},
    )
    start_halo.start()
    pl.loop(2, trips)(pipelined)
    start_halo.wait()
    put_raw(nb + 1, first_halo[...])
    for i in range(nb - unroll, nb):
        first_step(i)

    states = (state_a, state_b)
    for step in range(1, STEPS):
        now, later = states[step % 2], states[1 - step % 2]
        arrival = remote(
            now.at[pl.ds(3 * nb * BS, 2 * BS), :],
            halo.at[step],
            halo_send.at[step],
            halo_recv.at[step],
            {"depth": other},
        )
        arrival.start()
        for i in range(nb):
            if i == nb - unroll:
                arrival.wait()
                put(now, nb + 1, halo[step, :BS, :], halo[step, BS:, :])
            real, imag = advance(step, now, i)
            if step < STEPS - 1:
                put(later, i + 1, real, imag)
            else:
                final_real[rows_of(i, BS), :] = real
                final_imag[rows_of(i, BS), :] = imag
            if step == 1:
                for j in range(i * chips // nb, (i + 1) * chips // nb):
                    make_basis(j)

    def pick(owner, p):
        rows = owner * half + p * BS
        lhs = jnp.concatenate(
            [selector[pl.ds(pl.multiple_of(rows + i * 2 * half, BS), BS), :] for i in range(nb)], axis=1
        )
        rhs = jnp.concatenate([final_real[...], final_imag[...]], axis=1)
        x = dot(lhs, rhs).astype(BF16)
        return x[:, :BS], x[:, BS:]

    def swap(p):
        return remote(
            theirs.at[p], arrived.at[p], swap_send.at[p], swap_recv.at[p], {"depth": other}
        )

    def pair(p):
        return remote(own.at[p], mate.at[p], pair_send.at[p], pair_recv.at[p], {"freq": mate_id})

    for p in range(2):
        theirs[p, :BS, :], theirs[p, BS:, :] = pick(other, p)
    for p in range(2):
        swap(p).start()
    mine = [pick(depth, p) for p in range(2)]
    for p in range(2):
        swap(p).wait_recv()
        own[p, :BS, :] = mine[p][0] + arrived[p, :BS, :]
        own[p, BS:, :] = mine[p][1] + arrived[p, BS:, :]
        pair(p).start()

    targets = peers_of(chip, chips, 1)

    def outgoing(p, k):
        return remote(
            sums.at[p, targets[k]],
            inbox.at[p, k],
            out_send.at[p, k],
            out_recv.at[p, k],
            {"freq": 2 * targets[k] + core},
        )

    for p in range(2):
        pair(p).wait_recv()
        rhs = jnp.concatenate([own[p, :BS, :], own[p, BS:, :], mate[p, :BS, :], mate[p, BS:, :]], axis=1)
        group = min(8, chips)
        for g in range(chips // group):
            place = slice(g * group * span, (g + 1) * group * span)
            lhs = jnp.concatenate([basis[q, place, :] for q in range(4)], axis=1)
            part = (dot_nt(lhs, rhs) * factor).astype(BF16)
            for u in range(group):
                sums[p, g * group + u] = part[u * span : (u + 1) * span, :]
        for k in range(chips - 1):
            outgoing(p, k).start()

    for p in range(2):
        total = sums[p, chip].astype(F32)
        for k in range(chips - 1):
            outgoing(p, k).wait_recv()
        for k in range(chips - 1):
            total = total + inbox[p, k].astype(F32)
        out[:, p * BS : (p + 1) * BS] = total

    for p in range(2):
        swap(p).wait_send()
        pair(p).wait_send()
        for k in range(chips - 1):
            outgoing(p, k).wait_send()


def local(pressure_field, block_main, block_coupled, coupling, frequencies, receivers, floors):
    rows_here, width = pressure_field.shape
    nb = rows_here // BS
    unroll = min(8, nb // 2)
    count = receivers.shape[0]
    half = count // 2
    total_freq = frequencies.shape[0]
    chips = lax.axis_size("freq") // 2
    span = NT // (2 * chips)
    any_space = pl.BlockSpec(memory_space=pl.ANY)
    vmem = pl.BlockSpec(memory_space=pltpu.VMEM)
    smem = pl.BlockSpec(memory_space=pltpu.SMEM)
    dma = pltpu.SemaphoreType.DMA
    summed = pl.pallas_call(
        functools.partial(kernel, nb, unroll, chips, 1.0 / math.sqrt(total_freq)),
        out_shape=jax.ShapeDtypeStruct((span, half), F32),
        in_specs=[any_space] * 6 + [smem],
        out_specs=vmem,
        scratch_shapes=[
            pltpu.VMEM((rows_here, width), BF16),
            pltpu.VMEM((rows_here * 6, BS), BF16),
            pltpu.VMEM((rows_here * 6, BS), BF16),
            pltpu.VMEM((nb * 12 * BS, BS), BF16),
            pltpu.VMEM(((nb + 2) * 3 * BS, BS), BF16),
            pltpu.VMEM(((nb + 2) * 3 * BS, BS), BF16),
            pltpu.VMEM((rows_here, BS), BF16),
            pltpu.VMEM((rows_here, BS), BF16),
            pltpu.VMEM((nb * count, BS), BF16),
            pltpu.VMEM((count, BS), F32),
            pltpu.VMEM((8, width), F32),
            pltpu.VMEM((width, width), BF16),
            pltpu.VMEM((192, 192), BF16),
            pltpu.VMEM((BS, width), BF16),
            pltpu.VMEM((STEPS, 2 * BS, BS), BF16),
            pltpu.VMEM((2, 2 * BS, BS), BF16),
            pltpu.VMEM((2, 2 * BS, BS), BF16),
            pltpu.VMEM((2, 2 * BS, BS), BF16),
            pltpu.VMEM((2, 2 * BS, BS), BF16),
            pltpu.VMEM((4, NT // 2, BS), BF16),
            pltpu.VMEM((2, span, width), F32),
            pltpu.VMEM((2, chips, width), F32),
            pltpu.VMEM((2, chips, span, BS), BF16),
            pltpu.VMEM((2, chips, span, BS), BF16),
            pltpu.VMEM((1, width), F32),
            pltpu.VMEM((total_freq // BS, BS), F32),
            pltpu.VMEM((count // BS, BS), jnp.int32),
            dma((nb,)),
            dma((nb,)),
            dma((nb,)),
            dma((3,)),
            dma((STEPS,)),
            dma((STEPS,)),
            dma((2,)),
            dma((2,)),
            dma((2,)),
            dma((2,)),
            dma((2, chips)),
            dma((2, chips)),
        ],
        compiler_params=pltpu.CompilerParams(
            collective_id=0, has_side_effects=True, vmem_limit_bytes=60 * 1024 * 1024
        ),
        name="march",
    )(
        pressure_field,
        block_main.reshape(rows_here * 6, BS),
        block_coupled.reshape(rows_here * 6, BS),
        coupling.reshape(1, width),
        frequencies.reshape(total_freq // BS, BS),
        receivers.reshape(count // BS, BS),
        floors,
    )
    return summed.T


def solution(mesh):
    in_specs = (
        P("depth", "freq"),
        P("depth", None, None, None),
        P("depth", None, None, None),
        P("freq"),
        P(),
        P(),
        P(),
    )
    out_specs = P("depth", "freq")
    return jax.shard_map(local, mesh=mesh, in_specs=in_specs, out_specs=out_specs, check_vma=False)
```

```python
import functools
import math

import jax
import jax.numpy as jnp
from jax import lax
from jax.experimental import pallas as pl
from jax.experimental.pallas import tpu as pltpu
from jax.sharding import PartitionSpec as P

NT = 2048
STEPS = 4
BS = 128
MESH = pl.DeviceIdType.MESH
F32 = jnp.float32
BF16 = jnp.bfloat16


def iota(shape, dim):
    return lax.broadcasted_iota(jnp.int32, shape, dim)


def dot(a, b):
    return jnp.dot(a, b, preferred_element_type=F32)


def dot_nt(a, b):
    return lax.dot_general(a, b, (((1,), (1,)), ((), ())), preferred_element_type=F32)


def poly_coeffs():
    import numpy as np

    x = np.cos(np.pi * (np.arange(400) + 0.5) / 400) * 0.125 + 0.125
    y = np.sqrt(x)
    cheb_c = np.polynomial.chebyshev.Chebyshev.fit(x, np.cos(2 * np.pi * y), 8, domain=[0, 0.25])
    cheb_s = np.polynomial.chebyshev.Chebyshev.fit(x, np.sin(2 * np.pi * y) / y, 8, domain=[0, 0.25])
    to = np.polynomial.polynomial.Polynomial
    return (
        [float(v) for v in cheb_c.convert(kind=to).coef],
        [float(v) for v in cheb_s.convert(kind=to).coef],
    )


COS_COEFFS, SIN_COEFFS = poly_coeffs()


def horner(coeffs, z):
    total = jnp.full_like(z, coeffs[-1])
    for c in reversed(coeffs[:-1]):
        total = total * z + c
    return total


def cos_sin(turns):
    r = turns - jnp.floor(turns + 0.5)
    z = r * r
    return horner(COS_COEFFS, z), r * horner(SIN_COEFFS, z)


def torus_offsets(chips):
    if chips != 32:
        return None
    found = []
    for dx in range(4):
        for dy in range(4):
            for dh in range(2):
                if dx or dy or dh:
                    found.append((min(dx, 4 - dx) + min(dy, 4 - dy) + 2 * dh, dx, dy, dh))
    return [entry[1:] for entry in sorted(found, key=lambda entry: (-entry[0],) + entry[1:])]


def peers_of(chip, chips, sign):
    offsets = torus_offsets(chips)
    if offsets is None:
        return [(chip + sign * k + chips) % chips for k in range(1, chips)]
    x, y, h = chip // 8, (chip // 2) % 4, chip % 2
    return [
        (((x + sign * dx + 4) % 4) * 4 + (y + sign * dy + 4) % 4) * 2 + (h + dh) % 2
        for dx, dy, dh in offsets
    ]


def kernel(
    nb,
    chips,
    factor,
    field_hbm,
    main_hbm,
    side_hbm,
    coupling_hbm,
    frequencies_hbm,
    receivers_hbm,
    floors,
    out,
    raw_field,
    raw_main,
    raw_side,
    ops,
    state_a,
    state_b,
    final_real,
    final_imag,
    selector,
    recv_col,
    weights,
    split,
    order,
    first_halo,
    halo,
    theirs,
    arrived,
    own,
    mate,
    basis,
    near,
    far,
    sums,
    inbox,
    coupling,
    frequencies,
    receivers,
    field_sem,
    main_sem,
    side_sem,
    small_sem,
    halo_send,
    halo_recv,
    swap_send,
    swap_recv,
    pair_send,
    pair_recv,
    out_send,
    out_recv,
):
    depth, me = lax.axis_index("depth"), lax.axis_index("freq")
    other = 1 - depth
    chip, core = me // 2, me % 2
    mate_id = 2 * chip + (1 - core)
    width = 2 * BS
    first_row = depth * nb * BS
    half = 2 * BS
    span = NT // (2 * chips)

    def block_at(i):
        return jnp.where(depth == 0, i, nb - 1 - i)

    def rows_of(i, count):
        return pl.ds(pl.multiple_of(i * count, count), count)

    def field_copy(i):
        return pltpu.make_async_copy(
            field_hbm.at[rows_of(block_at(i), BS), :],
            raw_field.at[rows_of(i, BS), :],
            field_sem.at[i],
        )

    def op_copy(hbm, raw, sem, i):
        return pltpu.make_async_copy(
            hbm.at[rows_of(block_at(i), 6 * BS), :], raw.at[rows_of(i, 6 * BS), :], sem.at[i]
        )

    small = [
        pltpu.make_async_copy(coupling_hbm, coupling, small_sem.at[0]),
        pltpu.make_async_copy(receivers_hbm, receivers, small_sem.at[1]),
        pltpu.make_async_copy(frequencies_hbm, frequencies, small_sem.at[2]),
    ]
    for copy in small:
        copy.start()
    field_copy(nb - 1).start()

    @pl.loop(0, nb - 1)
    def _(i):
        field_copy(i).start()

    @pl.loop(0, nb)
    def _(i):
        op_copy(main_hbm, raw_main, main_sem, i).start()
        op_copy(side_hbm, raw_side, side_sem, i).start()

    barrier = pltpu.get_barrier_semaphore()

    def greet(target):
        pl.semaphore_signal(barrier, inc=1, device_id=target, device_id_type=MESH)

    greet({"depth": other})
    greet({"freq": mate_id})

    @pl.loop(1, chips)
    def _(k):
        greet({"freq": 2 * ((chip + k) % chips) + core})

    row, col = iota((width, width), 0), iota((width, width), 1)
    wanted = jnp.where(col < BS, 2 * col, 2 * (col - BS) + 1)
    split[...] = jnp.where(row == wanted, 1.0, 0.0).astype(BF16)
    row, col = iota((192, 192), 0), iota((192, 192), 1)
    k, c, d = row >> 6, (row >> 5) & 1, row & 31
    k = jnp.where(depth == 0, k, 2 - k)
    order[...] = jnp.where(col == 6 * d + 2 * k + c, 1.0, 0.0).astype(BF16)
    empty = jnp.zeros((3 * BS, BS), BF16)
    state_a[0 : 3 * BS, :] = empty
    state_b[0 : 3 * BS, :] = empty
    for copy in small:
        copy.wait()
    weights[...] = jnp.dot(
        jnp.broadcast_to(coupling[...], (8, width)),
        split[...].astype(F32),
        precision=lax.Precision.HIGHEST,
        preferred_element_type=F32,
    )
    spots = receivers[...].astype(F32)
    for g in range(receivers.shape[0]):
        tile = jnp.broadcast_to(spots[g : g + 1, :], (BS, BS))
        recv_col[g * BS : (g + 1) * BS, :] = tile.T

    freq = jnp.concatenate([frequencies[pl.ds(me, 1), :], frequencies[pl.ds(mate_id, 1), :]], axis=1)
    scale = 1.0 / NT
    near_n = iota((span, width), 0).astype(F32)
    near[0], near[1] = cos_sin(freq * near_n * scale)
    far_n = ((2 * iota((chips, width), 0) + core) * span).astype(F32)
    far[0], far[1] = cos_sin(freq * far_n * scale)

    def make_basis(j):
        ca, sa = far[0, j : j + 1, :], far[1, j : j + 1, :]
        cb, sb = near[0], near[1]
        real = (ca * cb - sa * sb).astype(BF16)
        imag = (-(sa * cb + ca * sb)).astype(BF16)
        for q, part in enumerate((real[:, :BS], imag[:, :BS], real[:, BS:], imag[:, BS:])):
            basis[q, j * span : (j + 1) * span, :] = part

    def put(state, slot, real, imag):
        state[rows_of(3 * slot, BS), :] = real
        state[rows_of(3 * slot + 1, BS), :] = imag
        state[rows_of(3 * slot + 2, BS), :] = -imag

    def remote(src, dst, send, recv, target):
        return pltpu.make_async_remote_copy(
            src_ref=src,
            dst_ref=dst,
            send_sem=send,
            recv_sem=recv,
            device_id=target,
            device_id_type=MESH,
        )

    def put_raw(slot, block):
        x = dot(block, split[...]).astype(BF16)
        put(state_a, slot, x[:, :BS], x[:, BS:])

    @pl.loop(0, nb)
    def _(i):
        field_copy(i).wait()

    for i in range(nb):
        put_raw(i + 1, raw_field[rows_of(i, BS), :])

    def bring_in(i):
        for q in range(4):
            part = pl.ds(pl.multiple_of(i * 6 * BS, 6 * BS) + 192 * q, 192)
            both = jnp.concatenate([raw_main[part, :], raw_side[part, :]], axis=1)
            sorted_rows = dot(order[...], both).astype(BF16)
            for kc in range(6):
                tile = sorted_rows[32 * kc : 32 * kc + 32, :]
                dest = pl.multiple_of(i * 12 * BS, 12 * BS) + kc * 2 * BS + 32 * q
                ops[pl.ds(dest, 32), :] = tile[:, :BS]
                ops[pl.ds(dest + BS, 32), :] = tile[:, BS:]

    def select(i):
        target = (first_row + block_at(i) * BS).astype(F32)
        lane = iota((2 * half, BS), 1).astype(F32) + target
        selector[rows_of(i, 2 * half), :] = jnp.where(recv_col[...] == lane, 1.0, 0.0).astype(BF16)

    def advance(step, state, i):
        lhs = jnp.concatenate([ops[rows_of(6 * i + kc, 2 * BS), :] for kc in range(6)], axis=1)
        tiles = []
        for slot in (i, i + 1, i + 2):
            real, imag, minus = (state[rows_of(3 * slot + q, BS), :] for q in range(3))
            tiles.append(jnp.concatenate([real, imag], axis=1))
            tiles.append(jnp.concatenate([minus, real], axis=1))
        product = dot(lhs, jnp.concatenate(tiles, axis=0))
        main, side = product[:BS], product[BS:]
        w_real, w_imag = weights[0:1, :BS], weights[0:1, BS:]
        side_real, side_imag = side[:, :BS], side[:, BS:]
        real = main[:, :BS] + (w_real * side_real - w_imag * side_imag)
        imag = main[:, BS:] + (w_real * side_imag + w_imag * side_real)
        depth_index = first_row + block_at(i) * BS + iota((BS, BS), 0)
        damping = jnp.where(depth_index >= floors[step], 0.5, 1.0).astype(F32)
        return (damping * real).astype(BF16), (damping * imag).astype(BF16)

    def load_group(first, last):
        for i in range(first, last):
            op_copy(main_hbm, raw_main, main_sem, i).wait()
            op_copy(side_hbm, raw_side, side_sem, i).wait()

    def first_step(i):
        put(state_b, i + 1, *advance(0, state_a, i))

    states = (state_a, state_b)

    def arrival(step):
        if step == 0:
            source, target = raw_field.at[rows_of(nb - 1, BS), :], first_halo
        else:
            source, target = states[step % 2].at[pl.ds(3 * nb * BS, 2 * BS), :], halo.at[step]
        return remote(source, target, halo_send.at[step], halo_recv.at[step], {"depth": other})

    bounds = [0, max(1, 3 * nb // 16), nb // 2, nb]
    load_group(0, bounds[1])
    for i in range(bounds[1]):
        bring_in(i)
        select(i)
    for g in (1, 2):
        load_group(bounds[g], bounds[g + 1])
        if g == 2:
            pl.semaphore_wait(barrier, chips + 1)
            arrival(0).start()
        ready, coming = bounds[g] - bounds[g - 1], bounds[g + 1] - bounds[g]
        done = 0
        for n in range(coming):
            bring_in(bounds[g] + n)
            select(bounds[g] + n)
            while done * coming < (n + 1) * ready:
                first_step(bounds[g - 1] + done)
                done += 1
    middle = bounds[2] + (nb - bounds[2]) // 2
    for i in range(bounds[2], middle):
        first_step(i)
    arrival(0).wait()
    put_raw(nb + 1, first_halo[...])
    first_step(nb - 1)
    arrival(1).start()
    for i in range(middle, nb - 1):
        first_step(i)

    for step in range(1, STEPS):
        now, later = states[step % 2], states[1 - step % 2]
        turn = nb - 1 if step == STEPS - 1 else nb - max(1, nb // (8 * step))
        for i in list(range(turn)) + [nb - 1] + list(range(turn, nb - 1)):
            if i == nb - 1:
                arrival(step).wait()
                put(now, nb + 1, halo[step, :BS, :], halo[step, BS:, :])
            real, imag = advance(step, now, i)
            if step < STEPS - 1:
                put(later, i + 1, real, imag)
            else:
                final_real[rows_of(i, BS), :] = real
                final_imag[rows_of(i, BS), :] = imag
            if i == nb - 1 and step < STEPS - 1:
                arrival(step + 1).start()
            if step == 1:
                for j in range(i * chips // nb, (i + 1) * chips // nb):
                    make_basis(j)

    def pick(owner, p):
        rows = owner * half + p * BS
        lhs = jnp.concatenate(
            [selector[pl.ds(pl.multiple_of(rows + i * 2 * half, BS), BS), :] for i in range(nb)], axis=1
        )
        rhs = jnp.concatenate([final_real[...], final_imag[...]], axis=1)
        x = dot(lhs, rhs).astype(BF16)
        return x[:, :BS], x[:, BS:]

    def swap(p):
        return remote(
            theirs.at[p], arrived.at[p], swap_send.at[p], swap_recv.at[p], {"depth": other}
        )

    def pair(p):
        return remote(own.at[p], mate.at[p], pair_send.at[p], pair_recv.at[p], {"freq": mate_id})

    for p in range(2):
        theirs[p, :BS, :], theirs[p, BS:, :] = pick(other, p)
    for p in range(2):
        swap(p).start()
    mine = [pick(depth, p) for p in range(2)]
    for p in range(2):
        swap(p).wait_recv()
        own[p, :BS, :] = mine[p][0] + arrived[p, :BS, :]
        own[p, BS:, :] = mine[p][1] + arrived[p, BS:, :]
        pair(p).start()

    targets = peers_of(chip, chips, 1)

    def outgoing(p, k):
        return remote(
            sums.at[p, targets[k]],
            inbox.at[p, k],
            out_send.at[p, k],
            out_recv.at[p, k],
            {"freq": 2 * targets[k] + core},
        )

    for p in range(2):
        pair(p).wait_recv()
        rhs = jnp.concatenate([own[p, :BS, :], own[p, BS:, :], mate[p, :BS, :], mate[p, BS:, :]], axis=1)
        group = min(8, chips)
        for g in range(chips // group):
            place = slice(g * group * span, (g + 1) * group * span)
            lhs = jnp.concatenate([basis[q, place, :] for q in range(4)], axis=1)
            part = (dot_nt(lhs, rhs) * factor).astype(BF16)
            for u in range(group):
                sums[p, g * group + u] = part[u * span : (u + 1) * span, :]
        for k in range(chips - 1):
            outgoing(p, k).start()

    for p in range(2):
        total = sums[p, chip].astype(F32)
        for k in range(chips - 1):
            outgoing(p, k).wait_recv()
        for k in range(chips - 1):
            total = total + inbox[p, k].astype(F32)
        out[:, p * BS : (p + 1) * BS] = total

    for p in range(2):
        swap(p).wait_send()
        pair(p).wait_send()
        for k in range(chips - 1):
            outgoing(p, k).wait_send()


def local(pressure_field, block_main, block_coupled, coupling, frequencies, receivers, floors):
    rows_here, width = pressure_field.shape
    nb = rows_here // BS
    count = receivers.shape[0]
    half = count // 2
    total_freq = frequencies.shape[0]
    chips = lax.axis_size("freq") // 2
    span = NT // (2 * chips)
    any_space = pl.BlockSpec(memory_space=pl.ANY)
    vmem = pl.BlockSpec(memory_space=pltpu.VMEM)
    smem = pl.BlockSpec(memory_space=pltpu.SMEM)
    dma = pltpu.SemaphoreType.DMA
    summed = pl.pallas_call(
        functools.partial(kernel, nb, chips, 1.0 / math.sqrt(total_freq)),
        out_shape=jax.ShapeDtypeStruct((span, half), F32),
        in_specs=[any_space] * 6 + [smem],
        out_specs=vmem,
        scratch_shapes=[
            pltpu.VMEM((rows_here, width), BF16),
            pltpu.VMEM((rows_here * 6, BS), BF16),
            pltpu.VMEM((rows_here * 6, BS), BF16),
            pltpu.VMEM((nb * 12 * BS, BS), BF16),
            pltpu.VMEM(((nb + 2) * 3 * BS, BS), BF16),
            pltpu.VMEM(((nb + 2) * 3 * BS, BS), BF16),
            pltpu.VMEM((rows_here, BS), BF16),
            pltpu.VMEM((rows_here, BS), BF16),
            pltpu.VMEM((nb * count, BS), BF16),
            pltpu.VMEM((count, BS), F32),
            pltpu.VMEM((8, width), F32),
            pltpu.VMEM((width, width), BF16),
            pltpu.VMEM((192, 192), BF16),
            pltpu.VMEM((BS, width), BF16),
            pltpu.VMEM((STEPS, 2 * BS, BS), BF16),
            pltpu.VMEM((2, 2 * BS, BS), BF16),
            pltpu.VMEM((2, 2 * BS, BS), BF16),
            pltpu.VMEM((2, 2 * BS, BS), BF16),
            pltpu.VMEM((2, 2 * BS, BS), BF16),
            pltpu.VMEM((4, NT // 2, BS), BF16),
            pltpu.VMEM((2, span, width), F32),
            pltpu.VMEM((2, chips, width), F32),
            pltpu.VMEM((2, chips, span, BS), BF16),
            pltpu.VMEM((2, chips, span, BS), BF16),
            pltpu.VMEM((1, width), F32),
            pltpu.VMEM((total_freq // BS, BS), F32),
            pltpu.VMEM((count // BS, BS), jnp.int32),
            dma((nb,)),
            dma((nb,)),
            dma((nb,)),
            dma((3,)),
            dma((STEPS,)),
            dma((STEPS,)),
            dma((2,)),
            dma((2,)),
            dma((2,)),
            dma((2,)),
            dma((2, chips)),
            dma((2, chips)),
        ],
        compiler_params=pltpu.CompilerParams(
            collective_id=0, has_side_effects=True, vmem_limit_bytes=60 * 1024 * 1024
        ),
        name="march",
    )(
        pressure_field,
        block_main.reshape(rows_here * 6, BS),
        block_coupled.reshape(rows_here * 6, BS),
        coupling.reshape(1, width),
        frequencies.reshape(total_freq // BS, BS),
        receivers.reshape(count // BS, BS),
        floors,
    )
    return summed.T


def solution(mesh):
    in_specs = (
        P("depth", "freq"),
        P("depth", None, None, None),
        P("depth", None, None, None),
        P("freq"),
        P(),
        P(),
        P(),
    )
    out_specs = P("depth", "freq")
    return jax.shard_map(local, mesh=mesh, in_specs=in_specs, out_specs=out_specs, check_vma=False)
```

```python
import functools
import math

import jax
import jax.numpy as jnp
from jax import lax
from jax.experimental import pallas as pl
from jax.experimental.pallas import tpu as pltpu
from jax.sharding import PartitionSpec as P

NT = 2048
STEPS = 4
BS = 128
MESH = pl.DeviceIdType.MESH
F32 = jnp.float32
BF16 = jnp.bfloat16


def iota(shape, dim):
    return lax.broadcasted_iota(jnp.int32, shape, dim)


def dot(a, b):
    return jnp.dot(a, b, preferred_element_type=F32)


def dot_nt(a, b):
    return lax.dot_general(a, b, (((1,), (1,)), ((), ())), preferred_element_type=F32)


def poly_coeffs():
    import numpy as np

    x = np.cos(np.pi * (np.arange(400) + 0.5) / 400) * 0.125 + 0.125
    y = np.sqrt(x)
    cheb_c = np.polynomial.chebyshev.Chebyshev.fit(x, np.cos(2 * np.pi * y), 8, domain=[0, 0.25])
    cheb_s = np.polynomial.chebyshev.Chebyshev.fit(x, np.sin(2 * np.pi * y) / y, 8, domain=[0, 0.25])
    to = np.polynomial.polynomial.Polynomial
    return (
        [float(v) for v in cheb_c.convert(kind=to).coef],
        [float(v) for v in cheb_s.convert(kind=to).coef],
    )


COS_COEFFS, SIN_COEFFS = poly_coeffs()


def horner(coeffs, z):
    total = jnp.full_like(z, coeffs[-1])
    for c in reversed(coeffs[:-1]):
        total = total * z + c
    return total


def cos_sin(turns):
    r = turns - jnp.floor(turns + 0.5)
    z = r * r
    return horner(COS_COEFFS, z), r * horner(SIN_COEFFS, z)


def torus_offsets(chips):
    if chips != 32:
        return None
    found = []
    for dx in range(4):
        for dy in range(4):
            for dh in range(2):
                if dx or dy or dh:
                    found.append((min(dx, 4 - dx) + min(dy, 4 - dy) + 2 * dh, dx, dy, dh))
    return [entry[1:] for entry in sorted(found, key=lambda entry: (-entry[0],) + entry[1:])]


def peers_of(chip, chips, sign):
    offsets = torus_offsets(chips)
    if offsets is None:
        return [(chip + sign * k + chips) % chips for k in range(1, chips)]
    x, y, h = chip // 8, (chip // 2) % 4, chip % 2
    return [
        (((x + sign * dx + 4) % 4) * 4 + (y + sign * dy + 4) % 4) * 2 + (h + dh) % 2
        for dx, dy, dh in offsets
    ]


def kernel(
    nb,
    chips,
    factor,
    field_hbm,
    main_hbm,
    side_hbm,
    coupling_hbm,
    frequencies_hbm,
    receivers_hbm,
    floors_hbm,
    out,
    raw_field,
    raw_main,
    raw_side,
    ops,
    state_a,
    state_b,
    final_real,
    final_imag,
    selector,
    recv_col,
    weights,
    split,
    order,
    first_halo,
    halo,
    theirs,
    arrived,
    own,
    mate,
    basis,
    near,
    far,
    sums,
    inbox,
    coupling,
    frequencies,
    receivers,
    floors,
    field_sem,
    main_sem,
    side_sem,
    small_sem,
    halo_send,
    halo_recv,
    swap_send,
    swap_recv,
    pair_send,
    pair_recv,
    out_send,
    out_recv,
):
    depth, me = lax.axis_index("depth"), lax.axis_index("freq")
    other = 1 - depth
    chip, core = me // 2, me % 2
    mate_id = 2 * chip + (1 - core)
    width = 2 * BS
    first_row = depth * nb * BS
    half = 2 * BS
    span = NT // (2 * chips)

    def block_at(i):
        return jnp.where(depth == 0, i, nb - 1 - i)

    def rows_of(i, count):
        return pl.ds(pl.multiple_of(i * count, count), count)

    def field_copy(i):
        return pltpu.make_async_copy(
            field_hbm.at[rows_of(block_at(i), BS), :],
            raw_field.at[rows_of(i, BS), :],
            field_sem,
        )

    bounds = [0, max(1, 3 * nb // 16), nb // 2, nb]

    def op_copy(hbm, raw, sem, i):
        return pltpu.make_async_copy(
            hbm.at[rows_of(block_at(i), 6 * BS), :], raw.at[rows_of(i, 6 * BS), :], sem
        )

    def wait_local(place, sem):
        pltpu.make_async_copy(place, place, sem).wait()

    small = [
        pltpu.make_async_copy(coupling_hbm, coupling, small_sem.at[0]),
        pltpu.make_async_copy(receivers_hbm, receivers, small_sem.at[1]),
        pltpu.make_async_copy(frequencies_hbm, frequencies, small_sem.at[2]),
        pltpu.make_async_copy(floors_hbm, floors, small_sem.at[3]),
    ]
    for copy in small:
        copy.start()
    @pl.loop(0, nb)
    def _(i):
        field_copy(i).start()

    for g in range(3):

        @pl.loop(bounds[g], bounds[g + 1])
        def _(i):
            op_copy(main_hbm, raw_main, main_sem.at[g], i).start()
            op_copy(side_hbm, raw_side, side_sem.at[g], i).start()

    barrier = pltpu.get_barrier_semaphore()

    def greet(target):
        pl.semaphore_signal(barrier, inc=1, device_id=target, device_id_type=MESH)

    greet({"depth": other})
    greet({"freq": mate_id})

    @pl.loop(1, chips)
    def _(k):
        greet({"freq": 2 * ((chip + k) % chips) + core})

    row, col = iota((width, width), 0), iota((width, width), 1)
    wanted = jnp.where(col < BS, 2 * col, 2 * (col - BS) + 1)
    split[...] = jnp.where(row == wanted, 1.0, 0.0).astype(BF16)
    row, col = iota((192, 192), 0), iota((192, 192), 1)
    k, c, d = row >> 6, (row >> 5) & 1, row & 31
    k = jnp.where(depth == 0, k, 2 - k)
    order[...] = jnp.where(col == 6 * d + 2 * k + c, 1.0, 0.0).astype(BF16)
    empty = jnp.zeros((3 * BS, BS), BF16)
    state_a[0 : 3 * BS, :] = empty
    state_b[0 : 3 * BS, :] = empty
    for copy in small:
        copy.wait()
    weights[...] = jnp.dot(
        jnp.broadcast_to(coupling[...], (8, width)),
        split[...].astype(F32),
        precision=lax.Precision.HIGHEST,
        preferred_element_type=F32,
    )
    spots = receivers[...].astype(F32)
    for g in range(receivers.shape[0]):
        tile = jnp.broadcast_to(spots[g : g + 1, :], (BS, BS))
        recv_col[g * BS : (g + 1) * BS, :] = tile.T

    freq = jnp.concatenate([frequencies[pl.ds(me, 1), :], frequencies[pl.ds(mate_id, 1), :]], axis=1)
    scale = 1.0 / NT
    near_n = iota((span, width), 0).astype(F32)
    near[0], near[1] = cos_sin(freq * near_n * scale)
    far_n = ((2 * iota((chips, width), 0) + core) * span).astype(F32)
    far[0], far[1] = cos_sin(freq * far_n * scale)

    def make_basis(j):
        ca, sa = far[0, j : j + 1, :], far[1, j : j + 1, :]
        cb, sb = near[0], near[1]
        real = (ca * cb - sa * sb).astype(BF16)
        imag = (-(sa * cb + ca * sb)).astype(BF16)
        for q, part in enumerate((real[:, :BS], imag[:, :BS], real[:, BS:], imag[:, BS:])):
            basis[q, j * span : (j + 1) * span, :] = part

    def put(state, slot, real, imag):
        state[rows_of(3 * slot, BS), :] = real
        state[rows_of(3 * slot + 1, BS), :] = imag
        state[rows_of(3 * slot + 2, BS), :] = -imag

    def remote(src, dst, send, recv, target):
        return pltpu.make_async_remote_copy(
            src_ref=src,
            dst_ref=dst,
            send_sem=send,
            recv_sem=recv,
            device_id=target,
            device_id_type=MESH,
        )

    def put_raw(slot, block):
        x = dot(block, split[...]).astype(BF16)
        put(state_a, slot, x[:, :BS], x[:, BS:])

    def bring_in(i):
        for q in range(4):
            part = pl.ds(pl.multiple_of(i * 6 * BS, 6 * BS) + 192 * q, 192)
            both = jnp.concatenate([raw_main[part, :], raw_side[part, :]], axis=1)
            sorted_rows = dot(order[...], both).astype(BF16)
            for kc in range(6):
                tile = sorted_rows[32 * kc : 32 * kc + 32, :]
                dest = pl.multiple_of(i * 12 * BS, 12 * BS) + kc * 2 * BS + 32 * q
                ops[pl.ds(dest, 32), :] = tile[:, :BS]
                ops[pl.ds(dest + BS, 32), :] = tile[:, BS:]

    def select(i):
        target = (first_row + block_at(i) * BS).astype(F32)
        lane = iota((2 * half, BS), 1).astype(F32) + target
        selector[rows_of(i, 2 * half), :] = jnp.where(recv_col[...] == lane, 1.0, 0.0).astype(BF16)

    def advance(step, state, i):
        lhs = jnp.concatenate([ops[rows_of(6 * i + kc, 2 * BS), :] for kc in range(6)], axis=1)
        tiles = []
        for slot in (i, i + 1, i + 2):
            real, imag, minus = (state[rows_of(3 * slot + q, BS), :] for q in range(3))
            tiles.append(jnp.concatenate([real, imag], axis=1))
            tiles.append(jnp.concatenate([minus, real], axis=1))
        product = dot(lhs, jnp.concatenate(tiles, axis=0))
        main, side = product[:BS], product[BS:]
        w_real, w_imag = weights[0:1, :BS], weights[0:1, BS:]
        side_real, side_imag = side[:, :BS], side[:, BS:]
        real = main[:, :BS] + (w_real * side_real - w_imag * side_imag)
        imag = main[:, BS:] + (w_real * side_imag + w_imag * side_real)
        depth_index = first_row + block_at(i) * BS + iota((BS, BS), 0)
        damping = jnp.where(depth_index >= floors[step], 0.5, 1.0).astype(F32)
        return (damping * real).astype(BF16), (damping * imag).astype(BF16)

    def load_group(g):
        rows = pl.ds(bounds[g] * 6 * BS, (bounds[g + 1] - bounds[g]) * 6 * BS)
        wait_local(raw_main.at[rows, :], main_sem.at[g])
        wait_local(raw_side.at[rows, :], side_sem.at[g])

    def first_step(i):
        put(state_b, i + 1, *advance(0, state_a, i))

    states = (state_a, state_b)

    def arrival(step):
        if step == 0:
            source, target = raw_field.at[rows_of(nb - 1, BS), :], first_halo
        else:
            source, target = states[step % 2].at[pl.ds(3 * nb * BS, 2 * BS), :], halo.at[step]
        return remote(source, target, halo_send.at[step], halo_recv.at[step], {"depth": other})

    wait_local(raw_field, field_sem)
    load_group(0)
    for i in range(nb):
        put_raw(i + 1, raw_field[rows_of(i, BS), :])
    for i in range(bounds[1]):
        bring_in(i)
        select(i)
    for g in (1, 2):
        load_group(g)
        if g == 2:
            pl.semaphore_wait(barrier, chips + 1)
            arrival(0).start()
        ready, coming = bounds[g] - bounds[g - 1], bounds[g + 1] - bounds[g]
        done = 0
        for n in range(coming):
            bring_in(bounds[g] + n)
            select(bounds[g] + n)
            while done * coming < (n + 1) * ready:
                first_step(bounds[g - 1] + done)
                done += 1
    middle = bounds[2] + (nb - bounds[2]) // 2
    for i in range(bounds[2], middle):
        first_step(i)
    arrival(0).wait()
    put_raw(nb + 1, first_halo[...])
    between = max(1, nb // 10)
    for i in [nb - 1] + list(range(middle, middle + between)):
        first_step(i)
    arrival(1).start()
    for i in range(middle + between, nb - 1):
        first_step(i)

    for step in range(1, STEPS):
        now, later = states[step % 2], states[1 - step % 2]
        turn = nb - 1 if step == STEPS - 1 else nb - 1 - between - (2 - step) * between
        for i in list(range(turn)) + [nb - 1] + list(range(turn, nb - 1)):
            if i == nb - 1:
                arrival(step).wait()
                put(now, nb + 1, halo[step, :BS, :], halo[step, BS:, :])
            real, imag = advance(step, now, i)
            if step < STEPS - 1:
                put(later, i + 1, real, imag)
            else:
                final_real[rows_of(i, BS), :] = real
                final_imag[rows_of(i, BS), :] = imag
            if i == turn + between - 1 and step < STEPS - 1:
                arrival(step + 1).start()
            if step == 1:
                for j in range(i * chips // nb, (i + 1) * chips // nb):
                    make_basis(j)

    def pick(owner, p):
        rows = owner * half + p * BS
        lhs = jnp.concatenate(
            [selector[pl.ds(pl.multiple_of(rows + i * 2 * half, BS), BS), :] for i in range(nb)], axis=1
        )
        rhs = jnp.concatenate([final_real[...], final_imag[...]], axis=1)
        x = dot(lhs, rhs).astype(BF16)
        return x[:, :BS], x[:, BS:]

    def swap(p):
        return remote(
            theirs.at[p], arrived.at[p], swap_send.at[p], swap_recv.at[p], {"depth": other}
        )

    def pair(p):
        return remote(own.at[p], mate.at[p], pair_send.at[p], pair_recv.at[p], {"freq": mate_id})

    for p in range(2):
        theirs[p, :BS, :], theirs[p, BS:, :] = pick(other, p)
    for p in range(2):
        swap(p).start()
    mine = [pick(depth, p) for p in range(2)]
    for p in range(2):
        swap(p).wait_recv()
        own[p, :BS, :] = mine[p][0] + arrived[p, :BS, :]
        own[p, BS:, :] = mine[p][1] + arrived[p, BS:, :]
        pair(p).start()

    targets = peers_of(chip, chips, 1)

    def outgoing(p, k):
        return remote(
            sums.at[p, targets[k]],
            inbox.at[p, k],
            out_send.at[p],
            out_recv.at[p],
            {"freq": 2 * targets[k] + core},
        )

    for p in range(2):
        pair(p).wait_recv()
        rhs = jnp.concatenate([own[p, :BS, :], own[p, BS:, :], mate[p, :BS, :], mate[p, BS:, :]], axis=1)
        group = min(8, chips)
        for g in range(chips // group):
            place = slice(g * group * span, (g + 1) * group * span)
            lhs = jnp.concatenate([basis[q, place, :] for q in range(4)], axis=1)
            part = (dot_nt(lhs, rhs) * factor).astype(BF16)
            for u in range(group):
                sums[p, g * group + u] = part[u * span : (u + 1) * span, :]
        for k in range(chips - 1):
            outgoing(p, k).start()

    for p in range(2):
        total = sums[p, chip].astype(F32)
        wait_local(inbox.at[p, pl.ds(0, chips - 1)], out_recv.at[p])
        for k in range(chips - 1):
            total = total + inbox[p, k].astype(F32)
        out[:, p * BS : (p + 1) * BS] = total

    for p in range(2):
        swap(p).wait_send()
        pair(p).wait_send()
        wait_local(inbox.at[p, pl.ds(0, chips - 1)], out_send.at[p])


def local(pressure_field, block_main, block_coupled, coupling, frequencies, receivers, floors):
    rows_here, width = pressure_field.shape
    nb = rows_here // BS
    count = receivers.shape[0]
    half = count // 2
    total_freq = frequencies.shape[0]
    chips = lax.axis_size("freq") // 2
    span = NT // (2 * chips)
    any_space = pl.BlockSpec(memory_space=pl.ANY)
    vmem = pl.BlockSpec(memory_space=pltpu.VMEM)
    dma = pltpu.SemaphoreType.DMA
    summed = pl.pallas_call(
        functools.partial(kernel, nb, chips, 1.0 / math.sqrt(total_freq)),
        out_shape=jax.ShapeDtypeStruct((span, half), F32),
        in_specs=[any_space] * 7,
        out_specs=vmem,
        scratch_shapes=[
            pltpu.VMEM((rows_here, width), BF16),
            pltpu.VMEM((rows_here * 6, BS), BF16),
            pltpu.VMEM((rows_here * 6, BS), BF16),
            pltpu.VMEM((nb * 12 * BS, BS), BF16),
            pltpu.VMEM(((nb + 2) * 3 * BS, BS), BF16),
            pltpu.VMEM(((nb + 2) * 3 * BS, BS), BF16),
            pltpu.VMEM((rows_here, BS), BF16),
            pltpu.VMEM((rows_here, BS), BF16),
            pltpu.VMEM((nb * count, BS), BF16),
            pltpu.VMEM((count, BS), F32),
            pltpu.VMEM((8, width), F32),
            pltpu.VMEM((width, width), BF16),
            pltpu.VMEM((192, 192), BF16),
            pltpu.VMEM((BS, width), BF16),
            pltpu.VMEM((STEPS, 2 * BS, BS), BF16),
            pltpu.VMEM((2, 2 * BS, BS), BF16),
            pltpu.VMEM((2, 2 * BS, BS), BF16),
            pltpu.VMEM((2, 2 * BS, BS), BF16),
            pltpu.VMEM((2, 2 * BS, BS), BF16),
            pltpu.VMEM((4, NT // 2, BS), BF16),
            pltpu.VMEM((2, span, width), F32),
            pltpu.VMEM((2, chips, width), F32),
            pltpu.VMEM((2, chips, span, BS), BF16),
            pltpu.VMEM((2, chips, span, BS), BF16),
            pltpu.VMEM((1, width), F32),
            pltpu.VMEM((total_freq // BS, BS), F32),
            pltpu.VMEM((count // BS, BS), jnp.int32),
            pltpu.SMEM((STEPS,), jnp.int32),
            dma,
            dma((3,)),
            dma((3,)),
            dma((4,)),
            dma((STEPS,)),
            dma((STEPS,)),
            dma((2,)),
            dma((2,)),
            dma((2,)),
            dma((2,)),
            dma((2,)),
            dma((2,)),
        ],
        compiler_params=pltpu.CompilerParams(
            collective_id=0, has_side_effects=True, vmem_limit_bytes=60 * 1024 * 1024
        ),
        name="march",
    )(
        pressure_field,
        block_main.reshape(rows_here * 6, BS),
        block_coupled.reshape(rows_here * 6, BS),
        coupling.reshape(1, width),
        frequencies.reshape(total_freq // BS, BS),
        receivers.reshape(count // BS, BS),
        floors,
    )
    return summed.T


def solution(mesh):
    in_specs = (
        P("depth", "freq"),
        P("depth", None, None, None),
        P("depth", None, None, None),
        P("freq"),
        P(),
        P(),
        P(),
    )
    out_specs = P("depth", "freq")
    return jax.shard_map(local, mesh=mesh, in_specs=in_specs, out_specs=out_specs, check_vma=False)
```

```python
import functools
import math

import jax
import jax.numpy as jnp
from jax import lax
from jax.experimental import pallas as pl
from jax.experimental.pallas import tpu as pltpu
from jax.sharding import PartitionSpec as P

NT = 2048
STEPS = 4
BS = 128
MESH = pl.DeviceIdType.MESH
F32 = jnp.float32
BF16 = jnp.bfloat16


def iota(shape, dim):
    return lax.broadcasted_iota(jnp.int32, shape, dim)


def dot(a, b):
    return jnp.dot(a, b, preferred_element_type=F32)


def dot_nt(a, b):
    return lax.dot_general(a, b, (((1,), (1,)), ((), ())), preferred_element_type=F32)


def poly_coeffs():
    import numpy as np

    x = np.cos(np.pi * (np.arange(400) + 0.5) / 400) * 0.125 + 0.125
    y = np.sqrt(x)
    cheb_c = np.polynomial.chebyshev.Chebyshev.fit(x, np.cos(2 * np.pi * y), 8, domain=[0, 0.25])
    cheb_s = np.polynomial.chebyshev.Chebyshev.fit(x, np.sin(2 * np.pi * y) / y, 8, domain=[0, 0.25])
    to = np.polynomial.polynomial.Polynomial
    return (
        [float(v) for v in cheb_c.convert(kind=to).coef],
        [float(v) for v in cheb_s.convert(kind=to).coef],
    )


COS_COEFFS, SIN_COEFFS = poly_coeffs()


def horner(coeffs, z):
    total = jnp.full_like(z, coeffs[-1])
    for c in reversed(coeffs[:-1]):
        total = total * z + c
    return total


def cos_sin(turns):
    r = turns - jnp.floor(turns + 0.5)
    z = r * r
    return horner(COS_COEFFS, z), r * horner(SIN_COEFFS, z)


def send_order(chips):
    if chips != 32:
        return list(range(chips))

    def reached(chip):
        x, y, h = chip // 8, (chip // 2) % 4, chip % 2
        return 1.25 * (x > 0) + 1.5 * (y > 0) + 2.0 * h + 0.01 * chip

    return sorted(range(chips), key=reached)


def kernel(
    nb,
    chips,
    factor,
    field_hbm,
    main_hbm,
    side_hbm,
    coupling_hbm,
    frequencies_hbm,
    receivers_hbm,
    floors_hbm,
    out,
    raw_field,
    raw_main,
    raw_side,
    ops,
    state_a,
    state_b,
    final_real,
    final_imag,
    selector,
    recv_col,
    weights,
    split,
    order,
    first_halo,
    halo,
    theirs,
    arrived,
    own,
    mate,
    basis,
    near,
    far,
    sums,
    inbox,
    coupling,
    frequencies,
    receivers,
    floors,
    field_sem,
    main_sem,
    side_sem,
    small_sem,
    halo_send,
    halo_recv,
    swap_send,
    swap_recv,
    pair_send,
    pair_recv,
    out_send,
    out_recv,
):
    depth, me = lax.axis_index("depth"), lax.axis_index("freq")
    other = 1 - depth
    chip, core = me // 2, me % 2
    mate_id = 2 * chip + (1 - core)
    width = 2 * BS
    first_row = depth * nb * BS
    half = 2 * BS
    span = NT // (2 * chips)

    def block_at(i):
        return jnp.where(depth == 0, i, nb - 1 - i)

    def rows_of(i, count):
        return pl.ds(pl.multiple_of(i * count, count), count)

    def field_copy(i):
        return pltpu.make_async_copy(
            field_hbm.at[rows_of(block_at(i), BS), :],
            raw_field.at[rows_of(i, BS), :],
            field_sem,
        )

    bounds = [0, max(1, 3 * nb // 16), nb // 2, nb]

    def op_copy(hbm, raw, sem, i):
        return pltpu.make_async_copy(
            hbm.at[rows_of(block_at(i), 6 * BS), :], raw.at[rows_of(i, 6 * BS), :], sem
        )

    def wait_local(place, sem):
        pltpu.make_async_copy(place, place, sem).wait()

    small = [
        pltpu.make_async_copy(coupling_hbm, coupling, small_sem.at[0]),
        pltpu.make_async_copy(receivers_hbm, receivers, small_sem.at[1]),
        pltpu.make_async_copy(frequencies_hbm, frequencies, small_sem.at[2]),
        pltpu.make_async_copy(floors_hbm, floors, small_sem.at[3]),
    ]
    for copy in small:
        copy.start()
    @pl.loop(0, nb)
    def _(i):
        field_copy(i).start()

    for g in range(3):

        @pl.loop(bounds[g], bounds[g + 1])
        def _(i):
            op_copy(main_hbm, raw_main, main_sem.at[g], i).start()
            op_copy(side_hbm, raw_side, side_sem.at[g], i).start()

    barrier = pltpu.get_barrier_semaphore()

    def greet(target):
        pl.semaphore_signal(barrier, inc=1, device_id=target, device_id_type=MESH)

    greet({"depth": other})
    greet({"freq": mate_id})

    @pl.loop(1, chips)
    def _(k):
        greet({"freq": 2 * ((chip + k) % chips) + core})

    row, col = iota((width, width), 0), iota((width, width), 1)
    wanted = jnp.where(col < BS, 2 * col, 2 * (col - BS) + 1)
    split[...] = jnp.where(row == wanted, 1.0, 0.0).astype(BF16)
    row, col = iota((192, 192), 0), iota((192, 192), 1)
    k, c, d = row >> 6, (row >> 5) & 1, row & 31
    k = jnp.where(depth == 0, k, 2 - k)
    order[...] = jnp.where(col == 6 * d + 2 * k + c, 1.0, 0.0).astype(BF16)
    empty = jnp.zeros((3 * BS, BS), BF16)
    state_a[0 : 3 * BS, :] = empty
    state_b[0 : 3 * BS, :] = empty
    for copy in small:
        copy.wait()
    weights[...] = jnp.dot(
        jnp.broadcast_to(coupling[...], (8, width)),
        split[...].astype(F32),
        precision=lax.Precision.HIGHEST,
        preferred_element_type=F32,
    )
    spots = receivers[...].astype(F32)
    for g in range(receivers.shape[0]):
        tile = jnp.broadcast_to(spots[g : g + 1, :], (BS, BS))
        recv_col[g * BS : (g + 1) * BS, :] = tile.T

    freq = jnp.concatenate([frequencies[pl.ds(me, 1), :], frequencies[pl.ds(mate_id, 1), :]], axis=1)
    scale = 1.0 / NT
    near_n = iota((span, width), 0).astype(F32)
    near[0], near[1] = cos_sin(freq * near_n * scale)
    far_n = ((2 * iota((chips, width), 0) + core) * span).astype(F32)
    far[0], far[1] = cos_sin(freq * far_n * scale)

    def make_basis(j):
        ca, sa = far[0, j : j + 1, :], far[1, j : j + 1, :]
        cb, sb = near[0], near[1]
        real = (ca * cb - sa * sb).astype(BF16)
        imag = (-(sa * cb + ca * sb)).astype(BF16)
        for q, part in enumerate((real[:, :BS], imag[:, :BS], real[:, BS:], imag[:, BS:])):
            basis[q, j * span : (j + 1) * span, :] = part

    def put(state, slot, real, imag):
        state[rows_of(3 * slot, BS), :] = real
        state[rows_of(3 * slot + 1, BS), :] = imag
        state[rows_of(3 * slot + 2, BS), :] = -imag

    def remote(src, dst, send, recv, target):
        return pltpu.make_async_remote_copy(
            src_ref=src,
            dst_ref=dst,
            send_sem=send,
            recv_sem=recv,
            device_id=target,
            device_id_type=MESH,
        )

    def put_raw(slot, block):
        x = dot(block, split[...]).astype(BF16)
        put(state_a, slot, x[:, :BS], x[:, BS:])

    def bring_in(i):
        for q in range(4):
            part = pl.ds(pl.multiple_of(i * 6 * BS, 6 * BS) + 192 * q, 192)
            both = jnp.concatenate([raw_main[part, :], raw_side[part, :]], axis=1)
            sorted_rows = dot(order[...], both).astype(BF16)
            for kc in range(6):
                tile = sorted_rows[32 * kc : 32 * kc + 32, :]
                dest = pl.multiple_of(i * 12 * BS, 12 * BS) + kc * 2 * BS + 32 * q
                ops[pl.ds(dest, 32), :] = tile[:, :BS]
                ops[pl.ds(dest + BS, 32), :] = tile[:, BS:]

    def select(i):
        target = (first_row + block_at(i) * BS).astype(F32)
        lane = iota((2 * half, BS), 1).astype(F32) + target
        selector[rows_of(i, 2 * half), :] = jnp.where(recv_col[...] == lane, 1.0, 0.0).astype(BF16)

    def advance(step, state, i):
        lhs = jnp.concatenate([ops[rows_of(6 * i + kc, 2 * BS), :] for kc in range(6)], axis=1)
        tiles = []
        for slot in (i, i + 1, i + 2):
            real, imag, minus = (state[rows_of(3 * slot + q, BS), :] for q in range(3))
            tiles.append(jnp.concatenate([real, imag], axis=1))
            tiles.append(jnp.concatenate([minus, real], axis=1))
        product = dot(lhs, jnp.concatenate(tiles, axis=0))
        main, side = product[:BS], product[BS:]
        w_real, w_imag = weights[0:1, :BS], weights[0:1, BS:]
        side_real, side_imag = side[:, :BS], side[:, BS:]
        real = main[:, :BS] + (w_real * side_real - w_imag * side_imag)
        imag = main[:, BS:] + (w_real * side_imag + w_imag * side_real)
        depth_index = first_row + block_at(i) * BS + iota((BS, BS), 0)
        damping = jnp.where(depth_index >= floors[step], 0.5, 1.0).astype(F32)
        return (damping * real).astype(BF16), (damping * imag).astype(BF16)

    def load_group(g):
        rows = pl.ds(bounds[g] * 6 * BS, (bounds[g + 1] - bounds[g]) * 6 * BS)
        wait_local(raw_main.at[rows, :], main_sem.at[g])
        wait_local(raw_side.at[rows, :], side_sem.at[g])

    def first_step(i):
        put(state_b, i + 1, *advance(0, state_a, i))

    states = (state_a, state_b)

    def arrival(step):
        if step == 0:
            source, target = raw_field.at[rows_of(nb - 1, BS), :], first_halo
        else:
            source, target = states[step % 2].at[pl.ds(3 * nb * BS, 2 * BS), :], halo.at[step]
        return remote(source, target, halo_send.at[step], halo_recv.at[step], {"depth": other})

    wait_local(raw_field, field_sem)
    for i in range(nb):
        put_raw(i + 1, raw_field[rows_of(i, BS), :])
    load_group(0)
    for i in range(bounds[1]):
        bring_in(i)
        select(i)
    for g in (1, 2):
        load_group(g)
        if g == 2:
            pl.semaphore_wait(barrier, chips + 1)
            arrival(0).start()
        ready, coming = bounds[g] - bounds[g - 1], bounds[g + 1] - bounds[g]
        done = 0
        for n in range(coming):
            bring_in(bounds[g] + n)
            select(bounds[g] + n)
            while done * coming < (n + 1) * ready:
                first_step(bounds[g - 1] + done)
                done += 1
    middle = bounds[2] + (nb - bounds[2]) // 2
    for i in range(bounds[2], middle):
        first_step(i)
    arrival(0).wait()
    put_raw(nb + 1, first_halo[...])
    between = max(1, nb // 10)
    for i in [nb - 1] + list(range(middle, middle + between)):
        first_step(i)
    arrival(1).start()
    for i in range(middle + between, nb - 1):
        first_step(i)

    for step in range(1, STEPS):
        now, later = states[step % 2], states[1 - step % 2]
        turn = nb - 1 if step == STEPS - 1 else nb - 1 - between - (2 - step) * between
        for i in list(range(turn)) + [nb - 1] + list(range(turn, nb - 1)):
            if i == nb - 1:
                arrival(step).wait()
                put(now, nb + 1, halo[step, :BS, :], halo[step, BS:, :])
            real, imag = advance(step, now, i)
            if step < STEPS - 1:
                put(later, i + 1, real, imag)
            else:
                final_real[rows_of(i, BS), :] = real
                final_imag[rows_of(i, BS), :] = imag
            if i == turn + between - 1 and step < STEPS - 1:
                arrival(step + 1).start()
            if step == 1:
                for j in range(i * chips // nb, (i + 1) * chips // nb):
                    make_basis(j)

    def pick(owner, p):
        rows = owner * half + p * BS
        lhs = jnp.concatenate(
            [selector[pl.ds(pl.multiple_of(rows + i * 2 * half, BS), BS), :] for i in range(nb)], axis=1
        )
        rhs = jnp.concatenate([final_real[...], final_imag[...]], axis=1)
        x = dot(lhs, rhs).astype(BF16)
        return x[:, :BS], x[:, BS:]

    def swap(p):
        return remote(
            theirs.at[p], arrived.at[p], swap_send.at[p], swap_recv.at[p], {"depth": other}
        )

    def pair(p):
        return remote(own.at[p], mate.at[p], pair_send.at[p], pair_recv.at[p], {"freq": mate_id})

    for p in range(2):
        theirs[p, :BS, :], theirs[p, BS:, :] = pick(other, p)
    for p in range(2):
        swap(p).start()
    mine = [pick(depth, p) for p in range(2)]
    for p in range(2):
        swap(p).wait_recv()
        own[p, :BS, :] = mine[p][0] + arrived[p, :BS, :]
        own[p, BS:, :] = mine[p][1] + arrived[p, BS:, :]
        pair(p).start()

    rhs = []
    for p in range(2):
        pair(p).wait_recv()
        parts = (own[p, :BS, :], own[p, BS:, :], mate[p, :BS, :], mate[p, BS:, :])
        rhs.append(jnp.concatenate(parts, axis=1))
    rhs = jnp.concatenate(rhs, axis=0)
    batch = min(8, chips)
    for g in range(chips // batch):
        place = slice(g * batch * span, (g + 1) * batch * span)
        lhs = jnp.concatenate([basis[q, place, :] for q in range(4)], axis=1)
        part = (dot_nt(lhs, rhs) * factor).astype(BF16)
        for u in range(batch):
            for p in range(2):
                sums[g * batch + u, p] = part[u * span : (u + 1) * span, p * BS : (p + 1) * BS]
    for target in send_order(chips):

        @pl.when(target != chip)
        def _():
            remote(
                sums.at[target], inbox.at[chip], out_send, out_recv, {"freq": 2 * target + core}
            ).start()

    inbox[chip] = sums[chip]
    received = inbox.at[pl.ds(0, chips - 1)]
    wait_local(received, out_recv)
    for p in range(2):
        total = inbox[0, p].astype(F32)
        for j in range(1, chips):
            total = total + inbox[j, p].astype(F32)
        out[:, p * BS : (p + 1) * BS] = total

    wait_local(received, out_send)
    for p in range(2):
        swap(p).wait_send()
        pair(p).wait_send()


def local(pressure_field, block_main, block_coupled, coupling, frequencies, receivers, floors):
    rows_here, width = pressure_field.shape
    nb = rows_here // BS
    count = receivers.shape[0]
    half = count // 2
    total_freq = frequencies.shape[0]
    chips = lax.axis_size("freq") // 2
    span = NT // (2 * chips)
    any_space = pl.BlockSpec(memory_space=pl.ANY)
    vmem = pl.BlockSpec(memory_space=pltpu.VMEM)
    dma = pltpu.SemaphoreType.DMA
    summed = pl.pallas_call(
        functools.partial(kernel, nb, chips, 1.0 / math.sqrt(total_freq)),
        out_shape=jax.ShapeDtypeStruct((span, half), F32),
        in_specs=[any_space] * 7,
        out_specs=vmem,
        scratch_shapes=[
            pltpu.VMEM((rows_here, width), BF16),
            pltpu.VMEM((rows_here * 6, BS), BF16),
            pltpu.VMEM((rows_here * 6, BS), BF16),
            pltpu.VMEM((nb * 12 * BS, BS), BF16),
            pltpu.VMEM(((nb + 2) * 3 * BS, BS), BF16),
            pltpu.VMEM(((nb + 2) * 3 * BS, BS), BF16),
            pltpu.VMEM((rows_here, BS), BF16),
            pltpu.VMEM((rows_here, BS), BF16),
            pltpu.VMEM((nb * count, BS), BF16),
            pltpu.VMEM((count, BS), F32),
            pltpu.VMEM((8, width), F32),
            pltpu.VMEM((width, width), BF16),
            pltpu.VMEM((192, 192), BF16),
            pltpu.VMEM((BS, width), BF16),
            pltpu.VMEM((STEPS, 2 * BS, BS), BF16),
            pltpu.VMEM((2, 2 * BS, BS), BF16),
            pltpu.VMEM((2, 2 * BS, BS), BF16),
            pltpu.VMEM((2, 2 * BS, BS), BF16),
            pltpu.VMEM((2, 2 * BS, BS), BF16),
            pltpu.VMEM((4, NT // 2, BS), BF16),
            pltpu.VMEM((2, span, width), F32),
            pltpu.VMEM((2, chips, width), F32),
            pltpu.VMEM((chips, 2, span, BS), BF16),
            pltpu.VMEM((chips, 2, span, BS), BF16),
            pltpu.VMEM((1, width), F32),
            pltpu.VMEM((total_freq // BS, BS), F32),
            pltpu.VMEM((count // BS, BS), jnp.int32),
            pltpu.SMEM((STEPS,), jnp.int32),
            dma,
            dma((3,)),
            dma((3,)),
            dma((4,)),
            dma((STEPS,)),
            dma((STEPS,)),
            dma((2,)),
            dma((2,)),
            dma((2,)),
            dma((2,)),
            dma,
            dma,
        ],
        compiler_params=pltpu.CompilerParams(
            collective_id=0, has_side_effects=True, vmem_limit_bytes=60 * 1024 * 1024
        ),
        name="march",
    )(
        pressure_field,
        block_main.reshape(rows_here * 6, BS),
        block_coupled.reshape(rows_here * 6, BS),
        coupling.reshape(1, width),
        frequencies.reshape(total_freq // BS, BS),
        receivers.reshape(count // BS, BS),
        floors,
    )
    return summed.T


def solution(mesh):
    in_specs = (
        P("depth", "freq"),
        P("depth", None, None, None),
        P("depth", None, None, None),
        P("freq"),
        P(),
        P(),
        P(),
    )
    out_specs = P("depth", "freq")
    return jax.shard_map(local, mesh=mesh, in_specs=in_specs, out_specs=out_specs, check_vma=False)
```

```python
import functools
import math

import jax
import jax.numpy as jnp
from jax import lax
from jax.experimental import pallas as pl
from jax.experimental.pallas import tpu as pltpu
from jax.sharding import PartitionSpec as P

NT = 2048
STEPS = 4
BS = 128
MESH = pl.DeviceIdType.MESH
F32 = jnp.float32
BF16 = jnp.bfloat16


def iota(shape, dim):
    return lax.broadcasted_iota(jnp.int32, shape, dim)


def dot(a, b):
    return jnp.dot(a, b, preferred_element_type=F32)


def dot_nt(a, b):
    return lax.dot_general(a, b, (((1,), (1,)), ((), ())), preferred_element_type=F32)


def poly_coeffs():
    import numpy as np

    x = np.cos(np.pi * (np.arange(400) + 0.5) / 400) * 0.125 + 0.125
    y = np.sqrt(x)
    cheb_c = np.polynomial.chebyshev.Chebyshev.fit(x, np.cos(2 * np.pi * y), 8, domain=[0, 0.25])
    cheb_s = np.polynomial.chebyshev.Chebyshev.fit(x, np.sin(2 * np.pi * y) / y, 8, domain=[0, 0.25])
    to = np.polynomial.polynomial.Polynomial
    return (
        [float(v) for v in cheb_c.convert(kind=to).coef],
        [float(v) for v in cheb_s.convert(kind=to).coef],
    )


COS_COEFFS, SIN_COEFFS = poly_coeffs()


def horner(coeffs, z):
    total = jnp.full_like(z, coeffs[-1])
    for c in reversed(coeffs[:-1]):
        total = total * z + c
    return total


def cos_sin(turns):
    r = turns - jnp.floor(turns + 0.5)
    z = r * r
    return horner(COS_COEFFS, z), r * horner(SIN_COEFFS, z)


def send_order(chips):
    if chips != 32:
        return list(range(chips))

    def reached(chip):
        x, y, h = chip // 8, (chip // 2) % 4, chip % 2
        return 1.25 * (x > 0) + 1.5 * (y > 0) + 2.0 * h + 0.01 * chip

    return sorted(range(chips), key=reached)


def kernel(
    nb,
    chips,
    factor,
    field_hbm,
    main_hbm,
    side_hbm,
    coupling_hbm,
    frequencies_hbm,
    receivers_hbm,
    floors_hbm,
    out,
    raw_field,
    raw_main,
    raw_side,
    ops,
    state_a,
    state_b,
    final_real,
    final_imag,
    selector,
    recv_col,
    weights,
    split,
    order,
    first_halo,
    halo,
    theirs,
    arrived,
    own,
    mate,
    basis,
    near,
    far,
    sums,
    inbox,
    coupling,
    frequencies,
    receivers,
    floors,
    field_sem,
    main_sem,
    side_sem,
    small_sem,
    halo_send,
    halo_recv,
    swap_send,
    swap_recv,
    pair_send,
    pair_recv,
    out_send,
    out_recv,
):
    depth, me = lax.axis_index("depth"), lax.axis_index("freq")
    other = 1 - depth
    chip, core = me // 2, me % 2
    mate_id = 2 * chip + (1 - core)
    width = 2 * BS
    first_row = depth * nb * BS
    half = 2 * BS
    span = NT // (2 * chips)

    def block_at(i):
        return jnp.where(depth == 0, i, nb - 1 - i)

    def rows_of(i, count):
        return pl.ds(pl.multiple_of(i * count, count), count)

    def field_copy(i):
        return pltpu.make_async_copy(
            field_hbm.at[rows_of(block_at(i), BS), :],
            raw_field.at[rows_of(i, BS), :],
            field_sem,
        )

    bounds = [0, max(1, 3 * nb // 16), nb // 2, nb]

    def op_copy(hbm, raw, sem, i):
        return pltpu.make_async_copy(
            hbm.at[rows_of(block_at(i), 6 * BS), :], raw.at[rows_of(i, 6 * BS), :], sem
        )

    def wait_local(place, sem):
        pltpu.make_async_copy(place, place, sem).wait()

    small = [
        pltpu.make_async_copy(coupling_hbm, coupling, small_sem.at[0]),
        pltpu.make_async_copy(receivers_hbm, receivers, small_sem.at[1]),
        pltpu.make_async_copy(frequencies_hbm, frequencies, small_sem.at[2]),
        pltpu.make_async_copy(floors_hbm, floors, small_sem.at[3]),
    ]
    for copy in small:
        copy.start()
    @pl.loop(0, nb)
    def _(i):
        field_copy(i).start()

    for g in range(3):

        @pl.loop(bounds[g], bounds[g + 1])
        def _(i):
            op_copy(main_hbm, raw_main, main_sem.at[g], i).start()
            op_copy(side_hbm, raw_side, side_sem.at[g], i).start()

    barrier = pltpu.get_barrier_semaphore()

    def greet(target):
        pl.semaphore_signal(barrier, inc=1, device_id=target, device_id_type=MESH)

    greet({"depth": other})
    greet({"freq": mate_id})

    @pl.loop(1, chips)
    def _(k):
        greet({"freq": 2 * ((chip + k) % chips) + core})

    row, col = iota((width, width), 0), iota((width, width), 1)
    wanted = jnp.where(col < BS, 2 * col, 2 * (col - BS) + 1)
    split[...] = jnp.where(row == wanted, 1.0, 0.0).astype(BF16)
    row, col = iota((192, 192), 0), iota((192, 192), 1)
    k, c, d = row >> 6, (row >> 5) & 1, row & 31
    k = jnp.where(depth == 0, k, 2 - k)
    order[...] = jnp.where(col == 6 * d + 2 * k + c, 1.0, 0.0).astype(BF16)
    empty = jnp.zeros((3 * BS, BS), BF16)
    state_a[0 : 3 * BS, :] = empty
    state_b[0 : 3 * BS, :] = empty
    for copy in small:
        copy.wait()
    weights[...] = jnp.dot(
        jnp.broadcast_to(coupling[...], (8, width)),
        split[...].astype(F32),
        precision=lax.Precision.HIGHEST,
        preferred_element_type=F32,
    )
    spots = receivers[...].astype(F32)
    for g in range(receivers.shape[0]):
        tile = jnp.broadcast_to(spots[g : g + 1, :], (BS, BS))
        recv_col[g * BS : (g + 1) * BS, :] = tile.T

    freq = jnp.concatenate([frequencies[pl.ds(me, 1), :], frequencies[pl.ds(mate_id, 1), :]], axis=1)
    scale = 1.0 / NT
    near_n = iota((span, width), 0).astype(F32)
    near[0], near[1] = cos_sin(freq * near_n * scale)
    far_n = ((2 * iota((chips, width), 0) + core) * span).astype(F32)
    far[0], far[1] = cos_sin(freq * far_n * scale)

    def make_basis(j):
        ca, sa = far[0, j : j + 1, :], far[1, j : j + 1, :]
        cb, sb = near[0], near[1]
        real = (ca * cb - sa * sb).astype(BF16)
        imag = (-(sa * cb + ca * sb)).astype(BF16)
        for q, part in enumerate((real[:, :BS], imag[:, :BS], real[:, BS:], imag[:, BS:])):
            basis[q, j * span : (j + 1) * span, :] = part

    def put(state, slot, real, imag):
        state[rows_of(3 * slot, BS), :] = real
        state[rows_of(3 * slot + 1, BS), :] = imag
        state[rows_of(3 * slot + 2, BS), :] = -imag

    def remote(src, dst, send, recv, target):
        return pltpu.make_async_remote_copy(
            src_ref=src,
            dst_ref=dst,
            send_sem=send,
            recv_sem=recv,
            device_id=target,
            device_id_type=MESH,
        )

    def put_raw(slot, block):
        x = dot(block, split[...]).astype(BF16)
        put(state_a, slot, x[:, :BS], x[:, BS:])

    def bring_in(i):
        for q in range(4):
            part = pl.ds(pl.multiple_of(i * 6 * BS, 6 * BS) + 192 * q, 192)
            both = jnp.concatenate([raw_main[part, :], raw_side[part, :]], axis=1)
            sorted_rows = dot(order[...], both).astype(BF16)
            for kc in range(6):
                tile = sorted_rows[32 * kc : 32 * kc + 32, :]
                dest = pl.multiple_of(i * 12 * BS, 12 * BS) + kc * 2 * BS + 32 * q
                ops[pl.ds(dest, 32), :] = tile[:, :BS]
                ops[pl.ds(dest + BS, 32), :] = tile[:, BS:]

    def select(i):
        target = (first_row + block_at(i) * BS).astype(F32)
        lane = iota((2 * half, BS), 1).astype(F32) + target
        selector[rows_of(i, 2 * half), :] = jnp.where(recv_col[...] == lane, 1.0, 0.0).astype(BF16)

    def advance(step, state, i):
        lhs = jnp.concatenate([ops[rows_of(6 * i + kc, 2 * BS), :] for kc in range(6)], axis=1)
        tiles = []
        for slot in (i, i + 1, i + 2):
            real, imag, minus = (state[rows_of(3 * slot + q, BS), :] for q in range(3))
            tiles.append(jnp.concatenate([real, imag], axis=1))
            tiles.append(jnp.concatenate([minus, real], axis=1))
        product = dot(lhs, jnp.concatenate(tiles, axis=0))
        main, side = product[:BS], product[BS:]
        w_real, w_imag = weights[0:1, :BS], weights[0:1, BS:]
        side_real, side_imag = side[:, :BS], side[:, BS:]
        real = main[:, :BS] + (w_real * side_real - w_imag * side_imag)
        imag = main[:, BS:] + (w_real * side_imag + w_imag * side_real)
        depth_index = first_row + block_at(i) * BS + iota((BS, BS), 0)
        damping = jnp.where(depth_index >= floors[step], 0.5, 1.0).astype(F32)
        return (damping * real).astype(BF16), (damping * imag).astype(BF16)

    def load_group(g):
        rows = pl.ds(bounds[g] * 6 * BS, (bounds[g + 1] - bounds[g]) * 6 * BS)
        wait_local(raw_main.at[rows, :], main_sem.at[g])
        wait_local(raw_side.at[rows, :], side_sem.at[g])

    def first_step(i):
        put(state_b, i + 1, *advance(0, state_a, i))

    states = (state_a, state_b)

    def arrival(step):
        if step == 0:
            source, target = raw_field.at[rows_of(nb - 1, BS), :], first_halo
        else:
            source, target = states[step % 2].at[pl.ds(3 * nb * BS, 2 * BS), :], halo.at[step]
        return remote(source, target, halo_send.at[step], halo_recv.at[step], {"depth": other})

    wait_local(raw_field, field_sem)
    for i in range(nb):
        put_raw(i + 1, raw_field[rows_of(i, BS), :])
    load_group(0)
    for i in range(bounds[1]):
        bring_in(i)
        select(i)
    for g in (1, 2):
        load_group(g)
        if g == 2:
            pl.semaphore_wait(barrier, chips + 1)
            arrival(0).start()
        ready, coming = bounds[g] - bounds[g - 1], bounds[g + 1] - bounds[g]
        done = 0
        for n in range(coming):
            bring_in(bounds[g] + n)
            select(bounds[g] + n)
            while done * coming < (n + 1) * ready:
                first_step(bounds[g - 1] + done)
                done += 1
    middle = bounds[2] + (nb - bounds[2]) // 2
    for i in range(bounds[2], middle):
        first_step(i)
    arrival(0).wait()
    put_raw(nb + 1, first_halo[...])
    between = max(1, nb // 10)
    for i in [nb - 1] + list(range(middle, middle + between)):
        first_step(i)
    arrival(1).start()
    for i in range(middle + between, nb - 1):
        first_step(i)

    for step in range(1, STEPS):
        now, later = states[step % 2], states[1 - step % 2]
        turn = nb - 1 if step == STEPS - 1 else nb - 1 - between - (2 - step) * between
        for i in list(range(turn)) + [turn, nb - 1][turn // (nb - 1) :] + list(range(turn + 1, nb - 1)):
            if i == turn:
                arrival(step).wait()
                put(now, nb + 1, halo[step, :BS, :], halo[step, BS:, :])
            real, imag = advance(step, now, i)
            if step < STEPS - 1:
                put(later, i + 1, real, imag)
            else:
                final_real[rows_of(i, BS), :] = real
                final_imag[rows_of(i, BS), :] = imag
            if i == turn + between - 1 and step < STEPS - 1:
                arrival(step + 1).start()
            if step == 1:
                for j in range(i * chips // nb, (i + 1) * chips // nb):
                    make_basis(j)

    def pick(owner, p):
        rows = owner * half + p * BS
        lhs = jnp.concatenate(
            [selector[pl.ds(pl.multiple_of(rows + i * 2 * half, BS), BS), :] for i in range(nb)], axis=1
        )
        rhs = jnp.concatenate([final_real[...], final_imag[...]], axis=1)
        x = dot(lhs, rhs).astype(BF16)
        return x[:, :BS], x[:, BS:]

    def swap(p):
        return remote(
            theirs.at[p], arrived.at[p], swap_send.at[p], swap_recv.at[p], {"depth": other}
        )

    def pair(p):
        return remote(own.at[p], mate.at[p], pair_send.at[p], pair_recv.at[p], {"freq": mate_id})

    for p in range(2):
        theirs[p, :BS, :], theirs[p, BS:, :] = pick(other, p)
    for p in range(2):
        swap(p).start()
    mine = [pick(depth, p) for p in range(2)]
    for p in range(2):
        swap(p).wait_recv()
        own[p, :BS, :] = mine[p][0] + arrived[p, :BS, :]
        own[p, BS:, :] = mine[p][1] + arrived[p, BS:, :]
        pair(p).start()

    rhs = []
    for p in range(2):
        pair(p).wait_recv()
        parts = (own[p, :BS, :], own[p, BS:, :], mate[p, :BS, :], mate[p, BS:, :])
        rhs.append(jnp.concatenate(parts, axis=1))
    rhs = jnp.concatenate(rhs, axis=0)
    batch = min(8, chips)
    for g in range(chips // batch):
        place = slice(g * batch * span, (g + 1) * batch * span)
        lhs = jnp.concatenate([basis[q, place, :] for q in range(4)], axis=1)
        part = (dot_nt(lhs, rhs) * factor).astype(BF16)
        for u in range(batch):
            for p in range(2):
                sums[g * batch + u, p] = part[u * span : (u + 1) * span, p * BS : (p + 1) * BS]
    for target in send_order(chips):

        @pl.when(target != chip)
        def _():
            remote(
                sums.at[target], inbox.at[chip], out_send, out_recv, {"freq": 2 * target + core}
            ).start()

    inbox[chip] = sums[chip]
    received = inbox.at[pl.ds(0, chips - 1)]
    wait_local(received, out_recv)
    for p in range(2):
        total = inbox[0, p].astype(F32)
        for j in range(1, chips):
            total = total + inbox[j, p].astype(F32)
        out[:, p * BS : (p + 1) * BS] = total

    wait_local(received, out_send)
    for p in range(2):
        swap(p).wait_send()
        pair(p).wait_send()


def local(pressure_field, block_main, block_coupled, coupling, frequencies, receivers, floors):
    rows_here, width = pressure_field.shape
    nb = rows_here // BS
    count = receivers.shape[0]
    half = count // 2
    total_freq = frequencies.shape[0]
    chips = lax.axis_size("freq") // 2
    span = NT // (2 * chips)
    any_space = pl.BlockSpec(memory_space=pl.ANY)
    vmem = pl.BlockSpec(memory_space=pltpu.VMEM)
    dma = pltpu.SemaphoreType.DMA
    summed = pl.pallas_call(
        functools.partial(kernel, nb, chips, 1.0 / math.sqrt(total_freq)),
        out_shape=jax.ShapeDtypeStruct((span, half), F32),
        in_specs=[any_space] * 7,
        out_specs=vmem,
        scratch_shapes=[
            pltpu.VMEM((rows_here, width), BF16),
            pltpu.VMEM((rows_here * 6, BS), BF16),
            pltpu.VMEM((rows_here * 6, BS), BF16),
            pltpu.VMEM((nb * 12 * BS, BS), BF16),
            pltpu.VMEM(((nb + 2) * 3 * BS, BS), BF16),
            pltpu.VMEM(((nb + 2) * 3 * BS, BS), BF16),
            pltpu.VMEM((rows_here, BS), BF16),
            pltpu.VMEM((rows_here, BS), BF16),
            pltpu.VMEM((nb * count, BS), BF16),
            pltpu.VMEM((count, BS), F32),
            pltpu.VMEM((8, width), F32),
            pltpu.VMEM((width, width), BF16),
            pltpu.VMEM((192, 192), BF16),
            pltpu.VMEM((BS, width), BF16),
            pltpu.VMEM((STEPS, 2 * BS, BS), BF16),
            pltpu.VMEM((2, 2 * BS, BS), BF16),
            pltpu.VMEM((2, 2 * BS, BS), BF16),
            pltpu.VMEM((2, 2 * BS, BS), BF16),
            pltpu.VMEM((2, 2 * BS, BS), BF16),
            pltpu.VMEM((4, NT // 2, BS), BF16),
            pltpu.VMEM((2, span, width), F32),
            pltpu.VMEM((2, chips, width), F32),
            pltpu.VMEM((chips, 2, span, BS), BF16),
            pltpu.VMEM((chips, 2, span, BS), BF16),
            pltpu.VMEM((1, width), F32),
            pltpu.VMEM((total_freq // BS, BS), F32),
            pltpu.VMEM((count // BS, BS), jnp.int32),
            pltpu.SMEM((STEPS,), jnp.int32),
            dma,
            dma((3,)),
            dma((3,)),
            dma((4,)),
            dma((STEPS,)),
            dma((STEPS,)),
            dma((2,)),
            dma((2,)),
            dma((2,)),
            dma((2,)),
            dma,
            dma,
        ],
        compiler_params=pltpu.CompilerParams(
            collective_id=0, has_side_effects=True, vmem_limit_bytes=60 * 1024 * 1024
        ),
        name="march",
    )(
        pressure_field,
        block_main.reshape(rows_here * 6, BS),
        block_coupled.reshape(rows_here * 6, BS),
        coupling.reshape(1, width),
        frequencies.reshape(total_freq // BS, BS),
        receivers.reshape(count // BS, BS),
        floors,
    )
    return summed.T


def solution(mesh):
    in_specs = (
        P("depth", "freq"),
        P("depth", None, None, None),
        P("depth", None, None, None),
        P("freq"),
        P(),
        P(),
        P(),
    )
    out_specs = P("depth", "freq")
    return jax.shard_map(local, mesh=mesh, in_specs=in_specs, out_specs=out_specs, check_vma=False)
```
